512 devices in a mesh: wx: 128 (over y, x, z_hi, core), ny: 4 (over z_lo).
Axes of the slice: x: 4, y: 8, z: 8 (z_hi: 2, z_lo: 4; z = z_hi * 4 + z_lo), core: 2. Of those that a mesh axis runs over, the one named last changes fastest.
Arguments:
- displacement: float32 [3, 512, 6, 512], P(None, 'wx', None, 'ny'), may hold values from -0.1 to 0.1
- velocity: float32 [3, 512, 6, 512], P(None, 'wx', None, 'ny'), may hold values from -1 to 1
- labels: int32 [512, 6, 512], P('wx', None, 'ny'), may hold values from 0 to 7
- bond_mask: int32 [61, 512, 6, 512], P(None, 'wx', None, 'ny'), may hold values 0 or 1
- stiffness: float32 [8], replicated, may hold values from 1 to 10
- critical: float32 [8], replicated, may hold values from 0.02 to 0.2
Outputs:
- final_displacement: float32 [3, 512, 6, 512], P(None, 'wx', None, 'ny')
- final_velocity: float32 [3, 512, 6, 512], P(None, 'wx', None, 'ny')
The draws below stay inside these ranges and needn't reach their ends.
All inputs are finite; a program needn't handle non-finite values. No bound on the sum of `bond_mask` on one device may be relied on, other than what follows from the above.
Results may differ from the reference program's by a relative error of at most 0.00002.
Values sent between devices are 32-bit elements; how exact they have to be, the bound alone decides.
No kernel may reach another device: no remote copies, remote signals or barrier semaphores. Data moves between devices by JAX's collectives and lax.ppermute only.
A program may use at most 64 MiB of HBM per device.

```python
import math
import jax
import jax.numpy as jnp

NZ = 6
STEPS = 3
MATS = 8
OFFSETS = 61
NX = 512
NY = 512


def touch_ends(result, stream_key, smallest, top_value):
    shape = result.shape
    index_at = [jax.random.randint(jax.random.fold_in(stream_key, axis), (), 0, shape[axis]) for axis in range(len(shape))]
    result = result.at[tuple(index_at)].set(smallest)
    longest = shape.index(max(shape))
    index_at[longest] = (index_at[longest] + 1) % shape[longest]
    return result.at[tuple(index_at)].set(top_value)


def block_levels(rng, extent, shards, smallest, largest):
    gain, own = 1.0, jax.random.fold_in(rng, 6)
    for dim, shards_of in shards:
        steps = jnp.exp(jax.random.uniform(jax.random.fold_in(own, dim), (shards_of,), jnp.float32, smallest / len(shards), largest / len(shards)))
        gain = gain * jnp.repeat(steps, extent[dim] // shards_of).reshape([-1 if axis == dim else 1 for axis in range(len(extent))])
    return gain


def scatter_about(stream_key, extent, width, limit, cuts=(), kind=jnp.bfloat16):
    values = jax.random.normal(stream_key, extent, jnp.float32) * width
    if len(cuts) > 0:
        values = block_levels(stream_key, extent, cuts, -0.22, 0.18) * values
    return jnp.clip(values, min=-limit, max=limit).astype(kind)


def setup_inputs(seed: int = 0) -> dict:
    streams_of = jax.random.split(jax.random.key(seed), 7)
    return {
        "displacement": scatter_about(streams_of[0], (3, NX, NZ, NY), 0.02, 0.1, ((1, 128), (3, 4)), jnp.float32),
        "velocity": scatter_about(streams_of[1], (3, NX, NZ, NY), 0.2, 1.0, ((1, 128), (3, 4)), jnp.float32),
        "labels": touch_ends(jax.random.randint(streams_of[2], (NX, NZ, NY), 0, MATS), jax.random.fold_in(streams_of[2], 1), 0, MATS - 1).astype(jnp.int32),
        "bond_mask": touch_ends((jax.random.randint(streams_of[3], (OFFSETS, NX, NZ, NY), 0, 10) < 9).astype(jnp.int32), jax.random.fold_in(streams_of[3], 1), 0, 1),
        "stiffness": jnp.clip(jnp.exp(jax.random.uniform(streams_of[4], (MATS,), jnp.float32, math.log(1.0), math.log(10.0))), 1.0, 10.0),
        "critical": jnp.clip(jnp.exp(jax.random.uniform(streams_of[5], (MATS,), jnp.float32, math.log(0.02), math.log(0.2))), 0.02, 0.2),
    }


time_step = 0.05

def bond_offsets():
    chosen = []
    for step_x in range(0, 4):
        for step_z in range(-3, 4):
            for step_y in range(-3, 4):
                if step_x * step_x + step_z * step_z + step_y * step_y <= 9:
                    if step_x > 0 or (step_x == 0 and (step_z > 0 or (step_z == 0 and step_y > 0))):
                        chosen.append((step_x, step_z, step_y))
    return chosen

def node_material(labels, stiffness, critical):
    modulus = jnp.zeros(labels.shape, jnp.float32)
    strain_limit = jnp.zeros(labels.shape, jnp.float32)
    for material in range(MATS):
        matches = labels == material
        modulus = jnp.where(matches, stiffness[material], modulus)
        strain_limit = jnp.where(matches, critical[material], strain_limit)
    return (modulus, strain_limit)

def pair_force(offset, source, target, modulus_here, modulus_there, limit_here, limit_there, intact):
    length = math.sqrt(offset[0] * offset[0] + offset[1] * offset[1] + offset[2] * offset[2])
    relative = [float(offset[component]) + target[component] - source[component] for component in range(3)]
    distance = jnp.sqrt(relative[0] * relative[0] + relative[1] * relative[1] + relative[2] * relative[2])
    stretch = (distance - length) / length
    pair_modulus = 2.0 * modulus_here * modulus_there / (modulus_here + modulus_there)
    pair_limit = 0.5 * (limit_here + limit_there)
    ratio = stretch / pair_limit
    magnitude = intact * pair_modulus * stretch / (1.0 + ratio * ratio) / (length * length)
    return jnp.stack([magnitude * part for part in relative])

def total_force(displacement, modulus, strain_limit, bond_mask):
    padded = jnp.pad(displacement, ((0, 0), (3, 3), (3, 3), (3, 3)))
    modulus_pad = jnp.pad(modulus, 3)
    limit_pad = jnp.pad(strain_limit, 3)
    index_x = jnp.arange(NX, dtype=jnp.int32).reshape(NX, 1, 1)
    index_z = jnp.arange(NZ, dtype=jnp.int32).reshape(1, NZ, 1)
    index_y = jnp.arange(NY, dtype=jnp.int32).reshape(1, 1, NY)
    spread = jnp.zeros(padded.shape, jnp.float32)
    force_here = jnp.zeros(displacement.shape, jnp.float32)
    for number, offset in enumerate(bond_offsets()):
        step_x, step_z, step_y = offset
        low_x, low_z, low_y = (3 + step_x, 3 + step_z, 3 + step_y)
        target = padded[:, low_x:low_x + NX, low_z:low_z + NZ, low_y:low_y + NY]
        modulus_there = modulus_pad[low_x:low_x + NX, low_z:low_z + NZ, low_y:low_y + NY]
        limit_there = limit_pad[low_x:low_x + NX, low_z:low_z + NZ, low_y:low_y + NY]
        inside = (index_x + step_x >= 0) & (index_x + step_x < NX)
        inside = inside & (index_z + step_z >= 0) & (index_z + step_z < NZ)
        inside = inside & (index_y + step_y >= 0) & (index_y + step_y < NY)
        intact = jnp.where(inside, bond_mask[number], 0).astype(jnp.float32)
        force = pair_force(offset, displacement, target, modulus, modulus_there, strain_limit, limit_there, intact)
        force_here = force_here + force
        spread = spread.at[:, low_x:low_x + NX, low_z:low_z + NZ, low_y:low_y + NY].add(-force)
    return force_here + spread[:, 3:3 + NX, 3:3 + NZ, 3:3 + NY]

def reference(displacement, velocity, labels, bond_mask, stiffness, critical):
    modulus, strain_limit = node_material(labels, stiffness, critical)
    for repeat in range(STEPS):
        force = total_force(displacement, modulus, strain_limit, bond_mask)
        velocity = velocity + time_step * force
        displacement = displacement + time_step * velocity
    return (displacement, velocity)
```

```python
import math

import jax
import jax.numpy as jnp
from jax import lax
from jax.experimental import pallas as pl
from jax.experimental.pallas import tpu as pltpu
from jax.sharding import PartitionSpec as P

STEPS = 3
MATS = 8
DT = 0.05
X, Z, Y = 4, 6, 128
R = X * Z
W = 9
G = 42
SLOTS = 4
F32 = jnp.float32


def bond_offsets():
    out = []
    for a in range(0, 4):
        for b in range(-3, 4):
            for c in range(-3, 4):
                if a * a + b * b + c * c <= 9:
                    if a > 0 or (a == 0 and (b > 0 or (b == 0 and c > 0))):
                        out.append((a, b, c))
    return out


OFFS = bond_offsets()
NB = len(OFFS)
CROSS = [k for k in range(NB) if OFFS[k][0] > 0]


def rows_of(k):
    return OFFS[k][0] * Z + OFFS[k][1]


PREV_AT = {}
_at = 0
for _k in CROSS:
    PREV_AT[_k] = _at
    _at += rows_of(_k)
PREV_ROWS = -(-_at // 8) * 8
STATE0 = 5 * R
UNITS = 18 + NB + len(CROSS)
YROWS = -(-UNITS // SLOTS) * 8
EDGE = 8
BLOCK = R + EDGE


def lanes(rows):
    return lax.broadcasted_iota(jnp.int32, (rows, Y), 1)


def roll(x, shift):
    shift %= Y
    return x if shift == 0 else pltpu.roll(x, shift, axis=1)


def params(n):
    return pltpu.CompilerParams(vmem_limit_bytes=n << 20)


def vmem(n):
    return [pl.BlockSpec(memory_space=pltpu.VMEM)] * n


def smem(n):
    return [pl.BlockSpec(memory_space=pltpu.SMEM)] * n


def shape(rows):
    return jax.ShapeDtypeStruct((rows, Y), F32)


def first_kernel(nwx, nny, stiff, crit, u, v, lab, mask, st, xf, v0, m_out, tmp):
    wx, ny = lax.axis_index("wx"), lax.axis_index("ny")
    for q in range(3):
        for x in range(X):
            st[q * R + x * Z : q * R + (x + 1) * Z, :] = u[pl.ds(q * R + x, Z, stride=X), :]
            v0[q * R + x * Z : q * R + (x + 1) * Z, :] = v[pl.ds(q * R + x, Z, stride=X), :]
    for x in range(X):
        tmp[x * Z : (x + 1) * Z, :] = lab[pl.ds(x, Z, stride=X), :]
    label = tmp[...]
    mod = jnp.zeros((R, Y), F32)
    lim = jnp.zeros((R, Y), F32)
    for t in range(MATS):
        hit = label == t
        mod = jnp.where(hit, stiff[t], mod)
        lim = jnp.where(hit, crit[t], lim)
    st[3 * R : 4 * R, :] = mod
    st[4 * R : 5 * R, :] = lim
    xf[0:STATE0, :] = st[...]
    row = lax.broadcasted_iota(jnp.int32, (R, Y), 0)
    zi = row % Z
    gx = wx * X + row // Z
    gy = ny * Y + lanes(R)
    for k, (a, b, c) in enumerate(OFFS):
        for x in range(X):
            m_out[k * R + x * Z : k * R + (x + 1) * Z, :] = mask[
                pl.ds(k * R + x, Z, stride=X), :
            ].astype(F32)
        ok = (zi + b >= 0) & (zi + b < Z) & (gx + a < nwx * X)
        if c:
            ok = ok & (gy + c >= 0) & (gy + c < nny * Y)
        m_out[k * R : (k + 1) * R, :] = jnp.where(ok, m_out[k * R : (k + 1) * R, :], 0.0)
        if a:
            o = rows_of(k)
            at = STATE0 + PREV_AT[k]
            xf[at : at + o, :] = m_out[(k + 1) * R - o : (k + 1) * R, :]
    if _at < PREV_ROWS:
        xf[STATE0 + _at : STATE0 + PREV_ROWS, :] = jnp.zeros((PREV_ROWS - _at, Y), F32)


def pack_kernel(st, rf, rb, v0, m, to_upper, to_lower, buf):
    def unit(n):
        if n < 15:
            s, q = (n // 3, n % 3) if n < 9 else (n % 3, 3 + (n - 9) // 3)
            return (rf, st, rb)[s][q * R : (q + 1) * R, :]
        if n < 18:
            return v0[(n - 15) * R : (n - 14) * R, :]
        if n < 18 + NB:
            return m[(n - 18) * R : (n - 17) * R, :]
        k = CROSS[n - 18 - NB]
        o = rows_of(k)
        at = (n - 18 - NB) * R
        buf[at : at + R - o, :] = jnp.zeros((R - o, Y), F32)
        buf[at + R - o : at + R, :] = rf[STATE0 + PREV_AT[k] : STATE0 + PREV_AT[k] + o, :]
        return buf[at : at + R, :]

    lane = lanes(8)
    for t in range(YROWS // 8):
        up = jnp.zeros((8, Y), F32)
        low = jnp.zeros((8, Y), F32)
        for p in range(SLOTS):
            if t * SLOTS + p >= UNITS:
                continue
            value = unit(t * SLOTS + p)
            for g in range(3):
                part = value[8 * g : 8 * g + 8, :]
                at = G * g + W * p
                here = (lane >= at) & (lane < at + W)
                up = jnp.where(here, roll(part, at + W), up)
                low = jnp.where(here, roll(part, at), low)
        to_upper[8 * t : 8 * t + 8, :] = up
        to_lower[8 * t : 8 * t + 8, :] = low


def expand(edge):
    lane = lanes(8)
    keep = (lane < W) | (lane >= Y - W)
    return [jnp.where(keep, roll(edge, Y - W - G * g), 0.0) for g in range(3)]


def spread_shifts(main, side, number, sh, qh, with_edge):
    rows = 3 * R
    lane = lanes(rows)
    for c in range(-3, 4):
        at = (number * 7 + c + 3) * rows
        if c == 0:
            moved, outer = main, side
        else:
            a, b = roll(main, -c), roll(side, -c)
            inner = (lane + c >= 0) & (lane + c < Y)
            moved, outer = jnp.where(inner, a, b), jnp.where(inner, b, a)
        sh[at : at + rows, :] = moved
        if with_edge:
            q = rows - 16
            ln = lanes(q)
            packed = jnp.where(
                ln < G,
                roll(outer[0:q, :], W),
                jnp.where(ln < 2 * G, roll(outer[8 : q + 8, :], G + W), roll(outer[16:, :], 2 * G + W)),
            )
            at = (number * 7 + c + 3) * q
            qh[at : at + q, :] = packed


def neighbours(sh, qh, number, o, c):
    rows, q = 3 * R, 3 * R - 16
    at = (number * 7 + c + 3) * rows + R + o
    main = sh[at : at + R, :]
    if qh is None:
        return main, None
    at = (number * 7 + c + 3) * q + R + o
    return main, qh[at : at + EDGE, :]


def pair_terms(d, here, there, kk, hh, length, acc):
    e = [there[q] + float(d[q]) - here[q] if d[q] else there[q] - here[q] for q in range(3)]
    t = jnp.sqrt(e[0] * e[0] + e[1] * e[1] + e[2] * e[2]) - length
    mag = kk * t / (hh + t * t)
    return [acc[q] + mag * e[q] for q in range(3)]


def forces(u_main, u_edge, sh, qh, kc, hc):
    acc = [jnp.zeros((R, Y), F32) for _ in range(3)]
    acc_e = [jnp.zeros((EDGE, Y), F32) for _ in range(3)]
    for k, off in enumerate(OFFS):
        length = math.sqrt(off[0] ** 2 + off[1] ** 2 + off[2] ** 2)
        for way in (0, 1):
            sign = 1 - 2 * way
            d = [sign * x for x in off]
            n = 2 * k + way
            both = [neighbours(sh, qh, q, sign * rows_of(k), d[2]) for q in range(3)]
            at = n * BLOCK
            acc = pair_terms(
                d, u_main, [x[0] for x in both], kc[at : at + R, :], hc[at : at + R, :], length, acc
            )
            if qh is not None:
                acc_e = pair_terms(
                    d, u_edge, [x[1] for x in both],
                    kc[at + R : at + BLOCK, :], hc[at + R : at + BLOCK, :], length, acc_e,
                )
    return acc, acc_e


def slab_sides(edges):
    return jnp.concatenate(sum([expand(e) for e in edges], []), axis=0)


def start_kernel(st, rf, rb, v0, m, rl, ru, kc, hc, s1, v1, sh, qh, tm0, tm1):
    lane = lanes(8)
    place = lane % G
    below = (place < W) & (lane < 3 * G)
    above = (place >= W) & (place < 2 * W) & (lane < 3 * G)

    def edge(n):
        t, p = n // SLOTS, n % SLOTS
        lo = roll(rl[8 * t : 8 * t + 8, :], -W * p)
        hi = roll(ru[8 * t : 8 * t + 8, :], W - W * p)
        return jnp.where(below, lo, jnp.where(above, hi, 0.0))

    def filled(x):
        return jnp.where(x > 0.0, x, 1.0)

    own_edge = []
    for q in range(5):
        at = q * R
        main = jnp.concatenate([rf[at : at + R, :], st[at : at + R, :], rb[at : at + R, :]], axis=0)
        edges = [edge(s * 3 + q) if q < 3 else edge(9 + 3 * (q - 3) + s) for s in range(3)]
        side = slab_sides(edges)
        if q >= 3:
            main, side = filled(main), filled(side)
        own_edge.append(edges[1] if q < 3 else filled(edges[1]))
        spread_shifts(main, side, q, sh, qh, True)

    mod, lim = st[3 * R : 4 * R, :], st[4 * R : 5 * R, :]
    mod_e, lim_e = own_edge[3], own_edge[4]

    def coefficients(mask, m_i, m_j, l_i, l_j, length):
        half = 0.5 * (l_i + l_j)
        sq = half * half
        kk = mask * (2.0 * m_i * m_j / (m_i + m_j)) * sq * (1.0 / length)
        return kk, sq * (length * length)

    cross = {k: i for i, k in enumerate(CROSS)}
    zero = jnp.zeros((R, Y), F32)
    for k, off in enumerate(OFFS):
        length = math.sqrt(off[0] ** 2 + off[1] ** 2 + off[2] ** 2)
        o, c = rows_of(k), off[2]
        mask = m[k * R : (k + 1) * R, :]
        mask_e = edge(18 + k)
        base = k * 2 * R
        tm0[base + R : base + 2 * R, :] = mask
        tm1[base + R : base + 2 * R, :] = slab_sides([mask_e])
        if o:
            tm0[base : base + R, :] = zero
            tm1[base : base + R, :] = zero
            if k in cross:
                tm0[base + R - o : base + R, :] = rf[
                    STATE0 + PREV_AT[k] : STATE0 + PREV_AT[k] + o, :
                ]
                tm1[base : base + R, :] = slab_sides([edge(18 + NB + cross[k])])
        a, b = tm0[base + R - o : base + 2 * R - o, :], tm1[base + R - o : base + 2 * R - o, :]
        if c:
            a, b = roll(a, c), roll(b, c)
            ln = lanes(R)
            inner = (ln - c >= 0) & (ln - c < Y)
            a, b = jnp.where(inner, a, b), jnp.where(inner, b, a)
        b_e = jnp.where(
            lane < G,
            roll(b[0:8, :], W),
            jnp.where(lane < 2 * G, roll(b[8:16, :], G + W), roll(b[16:24, :], 2 * G + W)),
        )
        for way, (mm, me) in enumerate(((mask, mask_e), (a, b_e))):
            sign = 1 - 2 * way
            mj, mj_e = neighbours(sh, qh, 3, sign * o, sign * c)
            lj, lj_e = neighbours(sh, qh, 4, sign * o, sign * c)
            at = (2 * k + way) * BLOCK
            kk, hh = coefficients(mm, mod, mj, lim, lj, length)
            kc[at : at + R, :] = kk
            hc[at : at + R, :] = hh
            kk, hh = coefficients(me, mod_e, mj_e, lim_e, lj_e, length)
            kc[at + R : at + BLOCK, :] = kk
            hc[at + R : at + BLOCK, :] = hh

    u_main = [st[q * R : (q + 1) * R, :] for q in range(3)]
    acc, acc_e = forces(u_main, own_edge[:3], sh, qh, kc, hc)
    for q in range(3):
        vel = v0[q * R : (q + 1) * R, :] + DT * acc[q]
        vel_e = edge(15 + q) + DT * acc_e[q]
        at = q * BLOCK
        v1[at : at + R, :] = vel
        v1[at + R : at + BLOCK, :] = vel_e
        s1[at : at + R, :] = u_main[q] + DT * vel
        s1[at + R : at + BLOCK, :] = own_edge[q] + DT * vel_e


def step_kernel(last, s, ra, rb, v, kc, hc, s_out, v_out, sh, qh, ext, side):
    even = lax.rem(lax.axis_index("wx"), 2) == 0
    for q in range(3):
        at = q * BLOCK
        top = jnp.where(even, rb[at : at + BLOCK, :], ra[at : at + BLOCK, :])
        end = jnp.where(even, ra[at : at + BLOCK, :], rb[at : at + BLOCK, :])
        mid = s[at : at + BLOCK, :]
        main = jnp.concatenate([top[:R], mid[:R], end[:R]], axis=0)
        sides = slab_sides([top[R:], mid[R:], end[R:]])
        spread_shifts(main, sides, q, sh, qh, not last)
    u_main = [s[q * BLOCK : q * BLOCK + R, :] for q in range(3)]
    u_edge = [s[q * BLOCK + R : (q + 1) * BLOCK, :] for q in range(3)]
    acc, acc_e = forces(u_main, u_edge, sh, None if last else qh, kc, hc)
    for q in range(3):
        at = q * BLOCK
        vel = v[at : at + R, :] + DT * acc[q]
        dis = u_main[q] + DT * vel
        if last:
            ext[q * R : (q + 1) * R, :] = dis
            side[q * R : (q + 1) * R, :] = vel
            for x in range(X):
                rows = slice(q * R + x * Z, q * R + (x + 1) * Z)
                s_out[pl.ds(q * R + x, Z, stride=X), :] = ext[rows, :]
                v_out[pl.ds(q * R + x, Z, stride=X), :] = side[rows, :]
        else:
            v_out[at : at + R, :] = vel
            s_out[at : at + R, :] = dis
            vel_e = v[at + R : at + BLOCK, :] + DT * acc_e[q]
            v_out[at + R : at + BLOCK, :] = vel_e
            s_out[at + R : at + BLOCK, :] = u_edge[q] + DT * vel_e


def on_device(nwx, nny, displacement, velocity, labels, bond_mask, stiffness, critical):
    import functools

    flat = lambda x: x.transpose(0, 2, 1, 3).reshape(-1, Y)
    u, v, mask = flat(displacement), flat(velocity), flat(bond_mask)
    lab = labels.transpose(1, 0, 2).reshape(R, Y)
    st, xf, v0, m = pl.pallas_call(
        functools.partial(first_kernel, nwx, nny),
        out_shape=(shape(STATE0), shape(STATE0 + PREV_ROWS), shape(3 * R), shape(NB * R)),
        in_specs=smem(2) + vmem(4),
        out_specs=tuple(vmem(4)),
        scratch_shapes=[pltpu.VMEM((R, Y), jnp.int32)],
        compiler_params=params(16),
        name="first",
    )(stiffness, critical, u, v, lab, mask)
    rf = lax.ppermute(xf, "wx", [(i, i + 1) for i in range(nwx - 1)])
    rb = lax.ppermute(st, "wx", [(i + 1, i) for i in range(nwx - 1)])
    to_upper, to_lower = pl.pallas_call(
        pack_kernel,
        out_shape=(shape(YROWS), shape(YROWS)),
        in_specs=vmem(5),
        out_specs=tuple(vmem(2)),
        scratch_shapes=[pltpu.VMEM((len(CROSS) * R, Y), F32)],
        compiler_params=params(16),
        name="pack",
    )(st, rf, rb, v0, m)
    rl = lax.ppermute(to_upper, "ny", [(i, i + 1) for i in range(nny - 1)])
    ru = lax.ppermute(to_lower, "ny", [(i + 1, i) for i in range(nny - 1)])
    kc, hc, s, vel = pl.pallas_call(
        start_kernel,
        out_shape=(shape(2 * NB * BLOCK), shape(2 * NB * BLOCK), shape(3 * BLOCK), shape(3 * BLOCK)),
        in_specs=vmem(7),
        out_specs=tuple(vmem(4)),
        scratch_shapes=[
            pltpu.VMEM((5 * 7 * 3 * R, Y), F32),
            pltpu.VMEM((5 * 7 * (3 * R - 16), Y), F32),
            pltpu.VMEM((NB * 2 * R, Y), F32),
            pltpu.VMEM((NB * 2 * R, Y), F32),
        ],
        compiler_params=params(24),
        name="start",
    )(st, rf, rb, v0, m, rl, ru)
    near = [(i, i ^ 1) for i in range(nwx)]
    far = [(i, i + 1) for i in range(1, nwx - 1, 2)] + [(i + 1, i) for i in range(1, nwx - 1, 2)]
    for n in range(1, STEPS):
        last = n == STEPS - 1
        rb = lax.ppermute(s, "wx", far)
        ra = lax.ppermute(s, "wx", near)
        size = 3 * R if last else 3 * BLOCK
        s, vel = pl.pallas_call(
            functools.partial(step_kernel, last),
            out_shape=(shape(size), shape(size)),
            in_specs=vmem(6),
            out_specs=tuple(vmem(2)),
            scratch_shapes=[
                pltpu.VMEM((3 * 7 * 3 * R, Y), F32),
                pltpu.VMEM((3 * 7 * (3 * R - 16), Y), F32),
                pltpu.VMEM((3 * R, Y), F32),
                pltpu.VMEM((3 * R, Y), F32),
            ],
            compiler_params=params(16),
            name="last" if last else "middle",
        )(s, ra, rb, vel, kc, hc)
    back = lambda x: x.reshape(3, Z, X, Y).transpose(0, 2, 1, 3)
    return back(s), back(vel)


def solution(mesh):
    import functools

    wide = P(None, "wx", None, "ny")
    return jax.shard_map(
        functools.partial(on_device, mesh.shape["wx"], mesh.shape["ny"]),
        mesh=mesh,
        in_specs=(wide, wide, P("wx", None, "ny"), wide, P(), P()),
        out_specs=(wide, wide),
        check_vma=False,
    )
```

```python
import functools
import math

import jax
import jax.numpy as jnp
from jax import lax
from jax.experimental import pallas as pl
from jax.experimental.pallas import tpu as pltpu
from jax.sharding import PartitionSpec as P


STEPS = 3
MATS = 8
DT = 0.05
X, Z, Y = 4, 6, 128
R = X * Z
W = 9
G = 42
SLOTS = 4
F32 = jnp.float32


def bond_offsets():
    out = []
    for a in range(0, 4):
        for b in range(-3, 4):
            for c in range(-3, 4):
                if a * a + b * b + c * c <= 9:
                    if a > 0 or (a == 0 and (b > 0 or (b == 0 and c > 0))):
                        out.append((a, b, c))
    return out


OFFS = bond_offsets()
NB = len(OFFS)
CROSS = [k for k in range(NB) if OFFS[k][0] > 0]


def rows_of(k):
    return OFFS[k][0] * Z + OFFS[k][1]


PREV_AT = {}
_at = 0
for _k in CROSS:
    PREV_AT[_k] = _at
    _at += rows_of(_k)
PREV_ROWS = -(-_at // 8) * 8
STATE0 = 5 * R
UNITS = 18 + 2 * NB
YROWS = -(-UNITS // SLOTS) * 8
EDGE = 8
BLOCK = R + EDGE


def lanes(rows):
    return lax.broadcasted_iota(jnp.int32, (rows, Y), 1)


def roll(x, shift):
    shift %= Y
    return x if shift == 0 else pltpu.roll(x, shift, axis=1)


def params(n):
    return pltpu.CompilerParams(vmem_limit_bytes=n << 20)


def vmem(n):
    return [pl.BlockSpec(memory_space=pltpu.VMEM)] * n


def shape(rows):
    return jax.ShapeDtypeStruct((rows, Y), F32)


def first_kernel(nwx, nny, *refs):
    given, (st, xf, v0, m_out), local, sems = refs[:6], refs[6:10], refs[10:16], refs[16]
    tmp = refs[17]
    copies = [pltpu.make_async_copy(g, l, sems.at[i]) for i, (g, l) in enumerate(zip(given, local))]
    for copy in copies:
        copy.start()
    stiff, crit, u, v, lab, mask = local
    wx, ny = lax.axis_index("wx"), lax.axis_index("ny")
    for copy in copies[:5]:
        copy.wait()
    for q in range(3):
        for x in range(X):
            st[q * R + x * Z : q * R + (x + 1) * Z, :] = u[pl.ds(q * R + x, Z, stride=X), :]
            v0[q * R + x * Z : q * R + (x + 1) * Z, :] = v[pl.ds(q * R + x, Z, stride=X), :]
    for x in range(X):
        tmp[x * Z : (x + 1) * Z, :] = lab[pl.ds(x, Z, stride=X), :]
    label = tmp[...]
    mod = jnp.zeros((R, Y), F32)
    lim = jnp.zeros((R, Y), F32)
    for t in range(MATS):
        hit = label == t
        mod = jnp.where(hit, stiff[t], mod)
        lim = jnp.where(hit, crit[t], lim)
    st[3 * R : 4 * R, :] = mod
    st[4 * R : 5 * R, :] = lim
    xf[0:STATE0, :] = st[...]
    row = lax.broadcasted_iota(jnp.int32, (R, Y), 0)
    zi = row % Z
    gx = wx * X + row // Z
    gy = ny * Y + lanes(R)
    copies[5].wait()
    for k, (a, b, c) in enumerate(OFFS):
        for x in range(X):
            m_out[k * R + x * Z : k * R + (x + 1) * Z, :] = mask[
                pl.ds(k * R + x, Z, stride=X), :
            ].astype(F32)
        ok = (zi + b >= 0) & (zi + b < Z) & (gx + a < nwx * X)
        if c:
            ok = ok & (gy + c >= 0) & (gy + c < nny * Y)
        m_out[k * R : (k + 1) * R, :] = jnp.where(ok, m_out[k * R : (k + 1) * R, :], 0.0)
        if a:
            o = rows_of(k)
            at = STATE0 + PREV_AT[k]
            xf[at : at + o, :] = m_out[(k + 1) * R - o : (k + 1) * R, :]
    if _at < PREV_ROWS:
        xf[STATE0 + _at : STATE0 + PREV_ROWS, :] = jnp.zeros((PREV_ROWS - _at, Y), F32)


def pack_kernel(st, rf, rb, v0, m, to_upper, to_lower, im):
    def unit(n):
        if n < 15:
            s, q = (n // 3, n % 3) if n < 9 else (n % 3, 3 + (n - 9) // 3)
            return (rf, st, rb)[s][q * R : (q + 1) * R, :]
        if n < 18:
            return v0[(n - 15) * R : (n - 14) * R, :]
        k = (n - 18) % NB
        if n < 18 + NB:
            return m[k * R : (k + 1) * R, :]
        o, at = rows_of(k), k * R
        if o == 0:
            im[at : at + R, :] = m[at : at + R, :]
        else:
            if OFFS[k][0]:
                im[at : at + o, :] = rf[STATE0 + PREV_AT[k] : STATE0 + PREV_AT[k] + o, :]
            else:
                im[at : at + o, :] = jnp.zeros((o, Y), F32)
            im[at + o : at + R, :] = m[at : at + R - o, :]
        return im[at : at + R, :]

    lane = lanes(8)
    for t in range(YROWS // 8):
        up = jnp.zeros((8, Y), F32)
        low = jnp.zeros((8, Y), F32)
        for p in range(SLOTS):
            if t * SLOTS + p >= UNITS:
                continue
            value = unit(t * SLOTS + p)
            for g in range(3):
                part = value[8 * g : 8 * g + 8, :]
                at = G * g + W * p
                here = (lane >= at) & (lane < at + W)
                up = jnp.where(here, roll(part, at + W), up)
                low = jnp.where(here, roll(part, at), low)
        to_upper[8 * t : 8 * t + 8, :] = up
        to_lower[8 * t : 8 * t + 8, :] = low


OWN = 6


def places():
    lane = lanes(8)
    return lane % G, lane < 3 * G


def tied(main, edge, with_edge=True):
    lane = lanes(8)
    rows = []
    for g in range(3):
        part = main[8 * g : 8 * g + 8, :]
        low = roll(edge, -(G * g + W))
        high = roll(edge, -(G * g + W + 2 * OWN))
        rows.append(jnp.where(lane < 3, low, jnp.where(lane >= Y - 3, high, part)))
    if with_edge:
        place, inside = places()
        for g in range(3):
            part = main[8 * g : 8 * g + 8, :]
            here = inside & (lane >= G * g) & (lane < G * (g + 1))
            low = here & (place >= W + 3) & (place < W + OWN)
            high = here & (place >= W + OWN) & (place < W + OWN + 3)
            edge = jnp.where(low, roll(part, G * g + W), edge)
            edge = jnp.where(high, roll(part, G * g + W + 2 * OWN), edge)
    return jnp.concatenate(rows, axis=0), edge


def shift_slabs(main, number, sh):
    rows = 3 * R
    for c in range(-3, 4):
        at = (number * 7 + c + 3) * rows
        sh[at : at + rows, :] = roll(main, -c)


def shift_edges(edges, number, qh):
    q = 3 * R - 16
    lane = lanes(8)
    tiles = []
    for n in range(q // 8):
        part = [roll(edges[(n + g) // 3], G * (g - (n + g) % 3)) for g in range(3)]
        tiles.append(jnp.where(lane < G, part[0], jnp.where(lane < 2 * G, part[1], part[2])))
    for c in range(-3, 4):
        at = (number * 7 + c + 3) * q
        for n, tile in enumerate(tiles):
            qh[at + 8 * n : at + 8 * n + 8, :] = roll(tile, -c)


def slab_at(number, o, c):
    return (number * 7 + c + 3) * 3 * R + R + o


def edge_at(number, o, c):
    return (number * 7 + c + 3) * (3 * R - 16) + R + o


DIRECTED = [(n // 2, 1 - 2 * (n % 2)) for n in range(2 * NB)]


def in_parts(live, size, fn):
    for start in range(0, 2 * NB, size):
        pl.when(live)(functools.partial(fn, range(start, min(start + size, 2 * NB))))


def add_forces(numbers, here, shifted, at_of, rows, kc, hc, acc):
    total = [acc[q * rows : (q + 1) * rows, :] for q in range(3)]
    mine = [here[q] for q in range(3)]
    for n in numbers:
        k, sign = DIRECTED[n]
        a, b, c = OFFS[k]
        length = math.sqrt(a * a + b * b + c * c)
        d = (sign * a, sign * b, sign * c)
        e = []
        for q in range(3):
            at = at_of(q, sign * rows_of(k), d[2])
            there = shifted[at : at + rows, :]
            e.append(there + float(d[q]) - mine[q] if d[q] else there - mine[q])
        sq = e[0] * e[0] + e[1] * e[1] + e[2] * e[2]
        t = sq * lax.rsqrt(jnp.maximum(sq, 1e-36)) - length
        mag = kc[n * rows : (n + 1) * rows, :] * t / (hc[n * rows : (n + 1) * rows, :] + t * t)
        total = [total[q] + mag * e[q] for q in range(3)]
    for q in range(3):
        acc[q * rows : (q + 1) * rows, :] = total[q]


def coefficients(mask, m_i, m_j, l_i, l_j, length):
    half = 0.5 * (l_i + l_j)
    sq = half * half
    return mask * (2.0 * m_i * m_j / (m_i + m_j)) * sq * (1.0 / length), sq * (length * length)


def length_of(k):
    a, b, c = OFFS[k]
    return math.sqrt(a * a + b * b + c * c)


def filled(x):
    return jnp.where(x > 0.0, x, 1.0)


PART = 16
PART_EDGE = 64


def slab_kernel(nwx, st, rf, rb, v0, m, im, kc, hc, u1, v1, sh, acc):
    live = lax.axis_index("wx") < nwx
    for q in range(5):
        at = q * R
        main = jnp.concatenate([rf[at : at + R, :], st[at : at + R, :], rb[at : at + R, :]], axis=0)
        shift_slabs(filled(main) if q >= 3 else main, q, sh)
    acc[...] = jnp.zeros_like(acc)

    def part(numbers):
        mod, lim = st[3 * R : 4 * R, :], st[4 * R : 5 * R, :]
        for n in numbers:
            k, sign = DIRECTED[n]
            o, c = sign * rows_of(k), sign * OFFS[k][2]
            mask = m[k * R : (k + 1) * R, :] if sign > 0 else roll(im[k * R : (k + 1) * R, :], -c)
            mj, lj = (sh[slab_at(q, o, c) : slab_at(q, o, c) + R, :] for q in (3, 4))
            kk, hh = coefficients(mask, mod, mj, lim, lj, length_of(k))
            kc[n * R : (n + 1) * R, :] = kk
            hc[n * R : (n + 1) * R, :] = hh
        here = [st[q * R : (q + 1) * R, :] for q in range(3)]
        add_forces(numbers, here, sh, slab_at, R, kc, hc, acc)

    in_parts(live, PART, part)
    vel = v0[...] + DT * acc[...]
    v1[...] = vel
    u1[...] = st[0 : 3 * R, :] + DT * vel


def edge_kernel(nwx, rl, ru, mine_up, mine_low, u1, v1, kc, hc, s_out, v_out, qh, acc, ue):
    live = lax.axis_index("wx") < nwx
    place, inside = places()

    def edge(n):
        t, p = n // SLOTS, n % SLOTS
        at = slice(8 * t, 8 * t + 8)
        out = jnp.where(inside & (place < W), roll(rl[at, :], -W * p), 0.0)
        own = roll(mine_low[at, :], W - W * p)
        out = jnp.where(inside & (place >= W) & (place < W + OWN), own, out)
        own = roll(mine_up[at, :], 2 * OWN - W * p)
        out = jnp.where(inside & (place >= W + OWN) & (place < W + 2 * OWN), own, out)
        above = roll(ru[at, :], W + 2 * OWN - W * p)
        return jnp.where(
            inside & (place >= W + 2 * OWN) & (place < 2 * W + 2 * OWN), above, out
        )

    for q in range(5):
        tiles = [edge(s * 3 + q) if q < 3 else edge(9 + 3 * (q - 3) + s) for s in range(3)]
        if q >= 3:
            tiles = [filled(x) for x in tiles]
        ue[8 * q : 8 * q + 8, :] = tiles[1]
        shift_edges(tiles, q, qh)
    acc[...] = jnp.zeros_like(acc)

    def part(numbers):
        mod, lim = ue[24:32, :], ue[32:40, :]
        for n in numbers:
            k, sign = DIRECTED[n]
            o, c = sign * rows_of(k), sign * OFFS[k][2]
            mask = edge(18 + k) if sign > 0 else roll(edge(18 + NB + k), -c)
            mj, lj = (qh[edge_at(q, o, c) : edge_at(q, o, c) + EDGE, :] for q in (3, 4))
            kk, hh = coefficients(mask, mod, mj, lim, lj, length_of(k))
            kc[n * EDGE : (n + 1) * EDGE, :] = kk
            hc[n * EDGE : (n + 1) * EDGE, :] = hh
        here = [ue[q * EDGE : (q + 1) * EDGE, :] for q in range(3)]
        add_forces(numbers, here, qh, edge_at, EDGE, kc, hc, acc)

    in_parts(live, PART_EDGE // 2, part)
    for q in range(3):
        vel = edge(15 + q) + DT * acc[q * EDGE : (q + 1) * EDGE, :]
        dis = ue[q * EDGE : (q + 1) * EDGE, :] + DT * vel
        finish(q, u1[q * R : (q + 1) * R, :], dis, v1[q * R : (q + 1) * R, :], vel, s_out, v_out)


def finish(q, dis, dis_e, vel, vel_e, s_out, v_out):
    dis, dis_e = tied(dis, dis_e)
    at = q * BLOCK
    s_out[at : at + R, :] = dis
    s_out[at + R : at + BLOCK, :] = dis_e
    v_out[at : at + R, :] = vel
    v_out[at + R : at + BLOCK, :] = vel_e


def step_kernel(nwx, last, s, ra, rb, v, kc, hc, ke, he, s_out, v_out, sh, qh, acc, acc_e):
    wx = lax.axis_index("wx")
    live = wx < nwx
    even = lax.rem(wx, 2) == 0
    for q in range(3):
        at = q * BLOCK
        top = jnp.where(even, rb[at : at + BLOCK, :], ra[at : at + BLOCK, :])
        end = jnp.where(even, ra[at : at + BLOCK, :], rb[at : at + BLOCK, :])
        mid = s[at : at + BLOCK, :]
        shift_slabs(jnp.concatenate([top[:R], mid[:R], end[:R]], axis=0), q, sh)
        shift_edges([top[R:], mid[R:], end[R:]], q, qh)
    acc[...] = jnp.zeros_like(acc)
    acc_e[...] = jnp.zeros_like(acc_e)
    u_main = [s[q * BLOCK : q * BLOCK + R, :] for q in range(3)]
    u_edge = [s[q * BLOCK + R : (q + 1) * BLOCK, :] for q in range(3)]

    def slab_part(numbers):
        here = [s[q * BLOCK : q * BLOCK + R, :] for q in range(3)]
        add_forces(numbers, here, sh, slab_at, R, kc, hc, acc)

    def edge_part(numbers):
        here = [s[q * BLOCK + R : (q + 1) * BLOCK, :] for q in range(3)]
        add_forces(numbers, here, qh, edge_at, EDGE, ke, he, acc_e)

    in_parts(live, PART, slab_part)
    in_parts(live, PART_EDGE, edge_part)
    for q in range(3):
        at = q * BLOCK
        vel = v[at : at + R, :] + DT * acc[q * R : (q + 1) * R, :]
        dis = u_main[q] + DT * vel
        vel_e = v[at + R : at + BLOCK, :] + DT * acc_e[q * EDGE : (q + 1) * EDGE, :]
        dis_e = u_edge[q] + DT * vel_e
        if not last:
            finish(q, dis, dis_e, vel, vel_e, s_out, v_out)
            continue
        acc[q * R : (q + 1) * R, :] = tied(dis, dis_e, False)[0]
        for x in range(X):
            s_out[pl.ds(q * R + x, Z, stride=X), :] = acc[q * R + x * Z : q * R + (x + 1) * Z, :]
        sh[q * R : (q + 1) * R, :] = tied(vel, vel_e, False)[0]
        for x in range(X):
            v_out[pl.ds(q * R + x, Z, stride=X), :] = sh[q * R + x * Z : q * R + (x + 1) * Z, :]


def call(kernel, outs, specs, scratch, mib, args, flops=0):
    return pl.pallas_call(
        kernel,
        out_shape=tuple(shape(n) for n in outs),
        in_specs=specs,
        out_specs=tuple(vmem(len(outs))),
        scratch_shapes=scratch,
        compiler_params=params(mib),
        cost_estimate=pl.CostEstimate(flops=flops, bytes_accessed=0, transcendentals=0),
    )(*args)


def tall(rows, dtype=F32):
    return pltpu.VMEM((rows, Y), dtype)


def on_device(nwx, nny, displacement, velocity, labels, bond_mask, stiffness, critical):
    flat = lambda x: x.transpose(0, 2, 1, 3).reshape(-1, Y)
    u, v, mask = flat(displacement), flat(velocity), flat(bond_mask)
    lab = labels.transpose(1, 0, 2).reshape(R, Y)
    sh3, qh3 = 7 * 3 * R, 7 * (3 * R - 16)
    i32 = jnp.int32
    st, xf, v0, m = call(
        functools.partial(first_kernel, nwx, nny),
        (STATE0, STATE0 + PREV_ROWS, 3 * R, NB * R),
        [pl.BlockSpec(memory_space=pltpu.HBM)] * 6,
        [pltpu.SMEM((MATS,), F32), pltpu.SMEM((MATS,), F32), tall(3 * R), tall(3 * R),
         tall(R, i32), tall(NB * R, i32), pltpu.SemaphoreType.DMA((6,)), tall(R, i32)],
        16, tuple(pltpu.with_memory_space_constraint(x, pltpu.HBM) for x in (stiffness, critical, u, v, lab, mask)),
    )
    rf = lax.ppermute(xf, "wx", [(i, i + 1) for i in range(nwx - 1)])
    rb = lax.ppermute(st, "wx", [(i + 1, i) for i in range(nwx - 1)])
    to_upper, to_lower, im = call(
        pack_kernel, (YROWS, YROWS, NB * R), vmem(5), [], 16, (st, rf, rb, v0, m)
    )
    rl = lax.ppermute(to_upper, "ny", [(i, i + 1) for i in range(nny - 1)])
    ru = lax.ppermute(to_lower, "ny", [(i + 1, i) for i in range(nny - 1)])
    kc, hc, u1, v1 = call(
        functools.partial(slab_kernel, nwx),
        (2 * NB * R, 2 * NB * R, 3 * R, 3 * R), vmem(6), [tall(5 * sh3), tall(3 * R)],
        24, (st, rf, rb, v0, m, im), 50_000_000,
    )
    ke, he, s, vel = call(
        functools.partial(edge_kernel, nwx),
        (2 * NB * EDGE, 2 * NB * EDGE, 3 * BLOCK, 3 * BLOCK), vmem(6),
        [tall(5 * qh3), tall(3 * EDGE), tall(5 * EDGE)],
        16, (rl, ru, to_upper, to_lower, u1, v1),
    )
    near = [(i, i ^ 1) for i in range(nwx)]
    far = [(i, i + 1) for i in range(1, nwx - 1, 2)] + [(i + 1, i) for i in range(1, nwx - 1, 2)]
    for n in range(1, STEPS):
        last = n == STEPS - 1
        rb = lax.ppermute(s, "wx", far)
        ra = lax.ppermute(s, "wx", near)
        size = 3 * R if last else 3 * BLOCK
        s, vel = call(
            functools.partial(step_kernel, nwx, last),
            (size, size), vmem(8),
            [tall(3 * sh3), tall(3 * qh3), tall(3 * R), tall(3 * EDGE)],
            16, (s, ra, rb, vel, kc, hc, ke, he),
        )
    back = lambda x: x.reshape(3, Z, X, Y).transpose(0, 2, 1, 3)
    return back(s), back(vel)


def solution(mesh):
    wide = P(None, "wx", None, "ny")
    return jax.shard_map(
        functools.partial(on_device, mesh.shape["wx"], mesh.shape["ny"]),
        mesh=mesh,
        in_specs=(wide, wide, P("wx", None, "ny"), wide, P(), P()),
        out_specs=(wide, wide),
        check_vma=False,
    )
```

```python
import functools
import math

import jax
import jax.numpy as jnp
from jax import lax
from jax.experimental import pallas as pl
from jax.experimental.pallas import tpu as pltpu
from jax.sharding import PartitionSpec as P


STEPS = 3
MATS = 8
DT = 0.05
X, Z, Y = 4, 6, 128
R = X * Z
W = 9
G = 42
SLOTS = 4
F32 = jnp.float32


def bond_offsets():
    out = []
    for a in range(0, 4):
        for b in range(-3, 4):
            for c in range(-3, 4):
                if a * a + b * b + c * c <= 9:
                    if a > 0 or (a == 0 and (b > 0 or (b == 0 and c > 0))):
                        out.append((a, b, c))
    return out


OFFS = bond_offsets()
NB = len(OFFS)
CROSS = [k for k in range(NB) if OFFS[k][0] > 0]


def rows_of(k):
    return OFFS[k][0] * Z + OFFS[k][1]


PREV_AT = {}
_at = 0
for _k in CROSS:
    PREV_AT[_k] = _at
    _at += rows_of(_k)
PREV_ROWS = -(-_at // 8) * 8
STATE0 = 5 * R
UNITS_OWN = 8 + NB
UNITS_NEXT = 10 + NB
YROWS = -(-UNITS_NEXT // SLOTS) * 8
EDGE = 8
BLOCK = R + EDGE


def lanes(rows):
    return lax.broadcasted_iota(jnp.int32, (rows, Y), 1)


def roll(x, shift):
    shift %= Y
    return x if shift == 0 else pltpu.roll(x, shift, axis=1)


def params(n):
    return pltpu.CompilerParams(vmem_limit_bytes=n << 20)


def vmem(n):
    return [pl.BlockSpec(memory_space=pltpu.VMEM)] * n


def shape(rows):
    return jax.ShapeDtypeStruct((rows, Y), F32)


def first_kernel(nwx, nny, *refs):
    given, (st, xf, v0, m_out), local, sems = refs[:6], refs[6:10], refs[10:16], refs[16]
    tmp = refs[17]
    copies = [pltpu.make_async_copy(g, l, sems.at[i]) for i, (g, l) in enumerate(zip(given, local))]
    for copy in copies:
        copy.start()
    stiff, crit, u, v, lab, mask = local
    wx, ny = lax.axis_index("wx"), lax.axis_index("ny")
    for copy in copies[:5]:
        copy.wait()
    for q in range(3):
        for x in range(X):
            st[q * R + x * Z : q * R + (x + 1) * Z, :] = u[pl.ds(q * R + x, Z, stride=X), :]
            v0[q * R + x * Z : q * R + (x + 1) * Z, :] = v[pl.ds(q * R + x, Z, stride=X), :]
    for x in range(X):
        tmp[x * Z : (x + 1) * Z, :] = lab[pl.ds(x, Z, stride=X), :]
    label = tmp[...]
    mod = jnp.zeros((R, Y), F32)
    lim = jnp.zeros((R, Y), F32)
    for t in range(MATS):
        hit = label == t
        mod = jnp.where(hit, stiff[t], mod)
        lim = jnp.where(hit, crit[t], lim)
    st[3 * R : 4 * R, :] = mod
    st[4 * R : 5 * R, :] = lim
    xf[0:STATE0, :] = st[...]
    row = lax.broadcasted_iota(jnp.int32, (R, Y), 0)
    zi = row % Z
    gx = wx * X + row // Z
    gy = ny * Y + lanes(R)
    copies[5].wait()
    for k, (a, b, c) in enumerate(OFFS):
        for x in range(X):
            m_out[k * R + x * Z : k * R + (x + 1) * Z, :] = mask[
                pl.ds(k * R + x, Z, stride=X), :
            ].astype(F32)
        ok = (zi + b >= 0) & (zi + b < Z) & (gx + a < nwx * X)
        if c:
            ok = ok & (gy + c >= 0) & (gy + c < nny * Y)
        m_out[k * R : (k + 1) * R, :] = jnp.where(ok, m_out[k * R : (k + 1) * R, :], 0.0)
        if a:
            o = rows_of(k)
            at = STATE0 + PREV_AT[k]
            xf[at : at + o, :] = m_out[(k + 1) * R - o : (k + 1) * R, :]
    if _at < PREV_ROWS:
        xf[STATE0 + _at : STATE0 + PREV_ROWS, :] = jnp.zeros((PREV_ROWS - _at, Y), F32)


def pack_units(unit, units, to_upper, to_lower):
    lane = lanes(8)
    for t in range(YROWS // 8):
        up = jnp.zeros((8, Y), F32)
        low = jnp.zeros((8, Y), F32)
        for p in range(SLOTS):
            if t * SLOTS + p >= units:
                continue
            value = unit(t * SLOTS + p)
            for g in range(3):
                part = value[8 * g : 8 * g + 8, :]
                at = G * g + W * p
                here = (lane >= at) & (lane < at + W)
                up = jnp.where(here, roll(part, at + W), up)
                low = jnp.where(here, roll(part, at), low)
        to_upper[8 * t : 8 * t + 8, :] = up
        to_lower[8 * t : 8 * t + 8, :] = low


def pack_own_kernel(st, v0, m, to_upper, to_lower):
    def unit(n):
        if n < 5:
            return st[n * R : (n + 1) * R, :]
        if n < 8:
            return v0[(n - 5) * R : (n - 4) * R, :]
        return m[(n - 8) * R : (n - 7) * R, :]

    pack_units(unit, UNITS_OWN, to_upper, to_lower)


def pack_kernel(rf, rb, m, to_upper, to_lower, im):
    def unit(n):
        if n < 10:
            ref, q = (rf, rb)[n // 5], n % 5
            return ref[q * R : (q + 1) * R, :]
        k = n - 10
        o, at = rows_of(k), k * R
        if o == 0:
            im[at : at + R, :] = m[at : at + R, :]
        else:
            if OFFS[k][0]:
                im[at : at + o, :] = rf[STATE0 + PREV_AT[k] : STATE0 + PREV_AT[k] + o, :]
            else:
                im[at : at + o, :] = jnp.zeros((o, Y), F32)
            im[at + o : at + R, :] = m[at : at + R - o, :]
        return im[at : at + R, :]

    pack_units(unit, UNITS_NEXT, to_upper, to_lower)


def group_place(lo, hi):
    place, inside = places()
    return inside & (place >= lo) & (place < hi)


def own_columns(n, mine_up, mine_low, out):
    t, p = n // SLOTS, n % SLOTS
    at = slice(8 * t, 8 * t + 8)
    out = jnp.where(group_place(W, W + OWN), roll(mine_low[at, :], W - W * p), out)
    return jnp.where(group_place(W + OWN, W + 2 * OWN), roll(mine_up[at, :], 2 * OWN - W * p), out)


def outer_columns(n, rl, ru, out):
    t, p = n // SLOTS, n % SLOTS
    at = slice(8 * t, 8 * t + 8)
    out = jnp.where(group_place(0, W), roll(rl[at, :], -W * p), out)
    return jnp.where(
        group_place(W + 2 * OWN, 2 * W + 2 * OWN), roll(ru[at, :], W + 2 * OWN - W * p), out
    )


def unpack_kernel(rl, ru, up1, low1, up2, low2, own, beside):
    zero = jnp.zeros((8, Y), F32)
    for n in range(UNITS_OWN):
        own[8 * n : 8 * n + 8, :] = outer_columns(n, rl, ru, own_columns(n, up1, low1, zero))
    for n in range(UNITS_NEXT):
        beside[8 * n : 8 * n + 8, :] = own_columns(n, up2, low2, zero)


OWN = 6


def places():
    lane = lanes(8)
    return lane % G, lane < 3 * G


def tied(main, edge, with_edge=True):
    lane = lanes(8)
    rows = []
    for g in range(3):
        part = main[8 * g : 8 * g + 8, :]
        low = roll(edge, -(G * g + W))
        high = roll(edge, -(G * g + W + 2 * OWN))
        rows.append(jnp.where(lane < 3, low, jnp.where(lane >= Y - 3, high, part)))
    if with_edge:
        place, inside = places()
        for g in range(3):
            part = main[8 * g : 8 * g + 8, :]
            here = inside & (lane >= G * g) & (lane < G * (g + 1))
            low = here & (place >= W + 3) & (place < W + OWN)
            high = here & (place >= W + OWN) & (place < W + OWN + 3)
            edge = jnp.where(low, roll(part, G * g + W), edge)
            edge = jnp.where(high, roll(part, G * g + W + 2 * OWN), edge)
    return jnp.concatenate(rows, axis=0), edge


def shift_slabs(main, number, sh, first=0):
    rows = 3 * R
    for c in range(-3, 4):
        at = (number * 7 + c + 3) * rows + first
        sh[at : at + main.shape[0], :] = roll(main, -c)


def shift_edges(edges, number, qh):
    q = 3 * R - 16
    lane = lanes(8)
    tiles = []
    for n in range(q // 8):
        part = [roll(edges[(n + g) // 3], G * (g - (n + g) % 3)) for g in range(3)]
        tiles.append(jnp.where(lane < G, part[0], jnp.where(lane < 2 * G, part[1], part[2])))
    for c in range(-3, 4):
        at = (number * 7 + c + 3) * q
        for n, tile in enumerate(tiles):
            qh[at + 8 * n : at + 8 * n + 8, :] = roll(tile, -c)


def slab_at(number, o, c):
    return (number * 7 + c + 3) * 3 * R + R + o


def edge_at(number, o, c):
    return (number * 7 + c + 3) * (3 * R - 16) + R + o


DIRECTED = [(n // 2, 1 - 2 * (n % 2)) for n in range(2 * NB)]
ALL = list(range(2 * NB))


def in_parts(live, numbers, size, fn):
    for start in range(0, len(numbers), size):
        pl.when(live)(functools.partial(fn, numbers[start : start + size]))


def add_forces(numbers, here, shifted, at_of, rows, kc, hc, acc, lo=0, hi=None):
    hi = rows if hi is None else hi
    total = [acc[q * rows + lo : q * rows + hi, :] for q in range(3)]
    mine = [here(q)[lo:hi, :] if (lo, hi) == (0, rows) else here(q, lo, hi) for q in range(3)]
    for n in numbers:
        k, sign = DIRECTED[n]
        a, b, c = OFFS[k]
        length = math.sqrt(a * a + b * b + c * c)
        d = (sign * a, sign * b, sign * c)
        e = []
        for q in range(3):
            at = at_of(q, sign * rows_of(k), d[2])
            there = shifted[at + lo : at + hi, :]
            e.append(there + float(d[q]) - mine[q] if d[q] else there - mine[q])
        sq = e[0] * e[0] + e[1] * e[1] + e[2] * e[2]
        t = sq * lax.rsqrt(jnp.maximum(sq, 1e-36)) - length
        at = n * rows
        mag = kc[at + lo : at + hi, :] * t / (hc[at + lo : at + hi, :] + t * t)
        total = [total[q] + mag * e[q] for q in range(3)]
    for q in range(3):
        acc[q * rows + lo : q * rows + hi, :] = total[q]


def rows_from(ref, stride, start=0):
    def here(q, lo=0, hi=None):
        hi = R if hi is None else hi
        return ref[q * stride + start + lo : q * stride + start + hi, :]

    return here


def edges_from(ref, stride, start=0):
    return lambda q: ref[q * stride + start : q * stride + start + EDGE, :]


def coefficients(mask, m_i, m_j, l_i, l_j, length):
    half = 0.5 * (l_i + l_j)
    sq = half * half
    return mask * (2.0 * m_i * m_j / (m_i + m_j)) * sq * (1.0 / length), sq * (length * length)


def length_of(k):
    a, b, c = OFFS[k]
    return math.sqrt(a * a + b * b + c * c)


def filled(x):
    return jnp.where(x > 0.0, x, 1.0)


PART = 16
PART_EDGE = 64


def slab_kernel(nwx, st, rf, rb, v0, m, im, kc, hc, u1, v1, sh, acc):
    live = lax.axis_index("wx") < nwx
    for q in range(5):
        at = q * R
        main = jnp.concatenate([rf[at : at + R, :], st[at : at + R, :], rb[at : at + R, :]], axis=0)
        shift_slabs(filled(main) if q >= 3 else main, q, sh)
    acc[...] = jnp.zeros_like(acc)

    def part(numbers):
        mod, lim = st[3 * R : 4 * R, :], st[4 * R : 5 * R, :]
        for n in numbers:
            k, sign = DIRECTED[n]
            o, c = sign * rows_of(k), sign * OFFS[k][2]
            mask = m[k * R : (k + 1) * R, :] if sign > 0 else roll(im[k * R : (k + 1) * R, :], -c)
            mj, lj = (sh[slab_at(q, o, c) : slab_at(q, o, c) + R, :] for q in (3, 4))
            kk, hh = coefficients(mask, mod, mj, lim, lj, length_of(k))
            kc[n * R : (n + 1) * R, :] = kk
            hc[n * R : (n + 1) * R, :] = hh
        add_forces(numbers, rows_from(st, R), sh, slab_at, R, kc, hc, acc)

    in_parts(live, ALL, PART, part)
    vel = v0[...] + DT * acc[...]
    v1[...] = vel
    u1[...] = st[0 : 3 * R, :] + DT * vel


def edge_kernel(nwx, rl, ru, own, beside, u1, v1, kc, hc, s_out, v_out, qh, acc, ue):
    live = lax.axis_index("wx") < nwx

    def own_tile(n):
        return own[8 * n : 8 * n + 8, :]

    def tile(n):
        return outer_columns(n, rl, ru, beside[8 * n : 8 * n + 8, :])

    for q in range(5):
        tiles = [tile(q), own_tile(q), tile(5 + q)]
        if q >= 3:
            tiles = [filled(x) for x in tiles]
        ue[8 * q : 8 * q + 8, :] = tiles[1]
        shift_edges(tiles, q, qh)
    acc[...] = jnp.zeros_like(acc)

    def part(numbers):
        mod, lim = ue[24:32, :], ue[32:40, :]
        for n in numbers:
            k, sign = DIRECTED[n]
            o, c = sign * rows_of(k), sign * OFFS[k][2]
            mask = own_tile(8 + k) if sign > 0 else roll(tile(10 + k), -c)
            mj, lj = (qh[edge_at(q, o, c) : edge_at(q, o, c) + EDGE, :] for q in (3, 4))
            kk, hh = coefficients(mask, mod, mj, lim, lj, length_of(k))
            kc[n * EDGE : (n + 1) * EDGE, :] = kk
            hc[n * EDGE : (n + 1) * EDGE, :] = hh
        add_forces(numbers, edges_from(ue, EDGE), qh, edge_at, EDGE, kc, hc, acc)

    in_parts(live, ALL, PART_EDGE, part)
    for q in range(3):
        vel = own_tile(5 + q) + DT * acc[q * EDGE : (q + 1) * EDGE, :]
        dis = ue[q * EDGE : (q + 1) * EDGE, :] + DT * vel
        finish(q, u1[q * R : (q + 1) * R, :], dis, v1[q * R : (q + 1) * R, :], vel, s_out, v_out)


def finish(q, dis, dis_e, vel, vel_e, s_out, v_out):
    dis, dis_e = tied(dis, dis_e)
    at = q * BLOCK
    s_out[at : at + R, :] = dis
    s_out[at + R : at + BLOCK, :] = dis_e
    v_out[at : at + R, :] = vel
    v_out[at + R : at + BLOCK, :] = vel_e


def toward(sign):
    return {a: [n for n in ALL if DIRECTED[n][1] == sign and OFFS[n // 2][0] == a] for a in (1, 2, 3)}


def mid_kernel(s, near, kc, hc, ke, he, acc, acc_e, sh, qh):
    even = lax.rem(lax.axis_index("wx"), 2) == 0
    acc[...] = jnp.zeros_like(acc)
    acc_e[...] = jnp.zeros_like(acc_e)
    zero = jnp.zeros((EDGE, Y), F32)

    def build(far_sign):
        for q in range(3):
            at = q * BLOCK
            mid, other = s[at : at + BLOCK, :], near[at : at + BLOCK, :]
            if far_sign < 0:
                shift_slabs(jnp.concatenate([zero, mid[:R], other[:R]], axis=0), q, sh, R - 8)
                shift_edges([zero, mid[R:], other[R:]], q, qh)
            else:
                shift_slabs(jnp.concatenate([other[:R], mid[:R], zero], axis=0), q, sh)
                shift_edges([other[R:], mid[R:], zero], q, qh)

    for far_sign, side in ((-1, even), (1, jnp.logical_not(even))):
        pl.when(side)(functools.partial(build, far_sign))
        leaving = toward(far_sign)
        whole = [n for n in ALL if not any(n in x for x in leaving.values())]

        def slab_part(numbers):
            add_forces(numbers, rows_from(s, BLOCK), sh, slab_at, R, kc, hc, acc)

        def edge_part(numbers):
            add_forces(numbers, edges_from(s, BLOCK, R), qh, edge_at, EDGE, ke, he, acc_e)

        in_parts(side, whole, PART, slab_part)
        in_parts(side, whole, PART_EDGE, edge_part)
        for a in (1, 2, 3):
            lo, hi = (Z * a, R) if far_sign < 0 else (0, R - Z * a)

            def inner_part(numbers, lo=lo, hi=hi):
                add_forces(numbers, rows_from(s, BLOCK), sh, slab_at, R, kc, hc, acc, lo, hi)

            in_parts(side, leaving[a], PART, inner_part)


def far_kernel(last, s, near, far, v, part, part_e, kc, hc, ke, he, s_out, v_out, sh, qh, acc, acc_e):
    even = lax.rem(lax.axis_index("wx"), 2) == 0
    acc[...] = part[...]
    acc_e[...] = part_e[...]

    def side_part(far_sign):
        for q in range(3):
            at = q * BLOCK
            mid, close, other = (x[at : at + BLOCK, :] for x in (s, near, far))
            if far_sign < 0:
                shift_slabs(jnp.concatenate([other[:R], mid[:8]], axis=0), q, sh)
                shift_edges([other[R:], mid[R:], close[R:]], q, qh)
            else:
                shift_slabs(jnp.concatenate([mid[R - 8 : R], other[:R]], axis=0), q, sh, 2 * R - 8)
                shift_edges([close[R:], mid[R:], other[R:]], q, qh)
        leaving = toward(far_sign)
        for a in (1, 2, 3):
            lo, hi = (0, Z * a) if far_sign < 0 else (R - Z * a, R)
            add_forces(leaving[a], rows_from(s, BLOCK), sh, slab_at, R, kc, hc, acc, lo, hi)
        numbers = leaving[1] + leaving[2] + leaving[3]
        add_forces(numbers, edges_from(s, BLOCK, R), qh, edge_at, EDGE, ke, he, acc_e)

    for far_sign, side in ((-1, even), (1, jnp.logical_not(even))):
        pl.when(side)(functools.partial(side_part, far_sign))
    for q in range(3):
        at = q * BLOCK
        vel = v[at : at + R, :] + DT * acc[q * R : (q + 1) * R, :]
        dis = s[at : at + R, :] + DT * vel
        vel_e = v[at + R : at + BLOCK, :] + DT * acc_e[q * EDGE : (q + 1) * EDGE, :]
        dis_e = s[at + R : at + BLOCK, :] + DT * vel_e
        if not last:
            finish(q, dis, dis_e, vel, vel_e, s_out, v_out)
            continue
        acc[q * R : (q + 1) * R, :] = tied(dis, dis_e, False)[0]
        for x in range(X):
            s_out[pl.ds(q * R + x, Z, stride=X), :] = acc[q * R + x * Z : q * R + (x + 1) * Z, :]
        sh[q * R : (q + 1) * R, :] = tied(vel, vel_e, False)[0]
        for x in range(X):
            v_out[pl.ds(q * R + x, Z, stride=X), :] = sh[q * R + x * Z : q * R + (x + 1) * Z, :]


def call(kernel, outs, specs, scratch, mib, args, flops=0):
    return pl.pallas_call(
        kernel,
        out_shape=tuple(shape(n) for n in outs),
        in_specs=specs,
        out_specs=tuple(vmem(len(outs))),
        scratch_shapes=scratch,
        compiler_params=params(mib),
        cost_estimate=pl.CostEstimate(flops=flops, bytes_accessed=0, transcendentals=0),
    )(*args)


def tall(rows, dtype=F32):
    return pltpu.VMEM((rows, Y), dtype)


def on_device(nwx, nny, displacement, velocity, labels, bond_mask, stiffness, critical):
    flat = lambda x: x.transpose(0, 2, 1, 3).reshape(-1, Y)
    u, v, mask = flat(displacement), flat(velocity), flat(bond_mask)
    lab = labels.transpose(1, 0, 2).reshape(R, Y)
    sh3, qh3 = 7 * 3 * R, 7 * (3 * R - 16)
    i32 = jnp.int32
    st, xf, v0, m = call(
        functools.partial(first_kernel, nwx, nny),
        (STATE0, STATE0 + PREV_ROWS, 3 * R, NB * R),
        [pl.BlockSpec(memory_space=pltpu.HBM)] * 6,
        [pltpu.SMEM((MATS,), F32), pltpu.SMEM((MATS,), F32), tall(3 * R), tall(3 * R),
         tall(R, i32), tall(NB * R, i32), pltpu.SemaphoreType.DMA((6,)), tall(R, i32)],
        16, tuple(pltpu.with_memory_space_constraint(x, pltpu.HBM) for x in (stiffness, critical, u, v, lab, mask)),
    )
    up = [(i, i + 1) for i in range(nny - 1)]
    down = [(i + 1, i) for i in range(nny - 1)]
    rf = lax.ppermute(xf, "wx", [(i, i + 1) for i in range(nwx - 1)])
    rb = lax.ppermute(st, "wx", [(i + 1, i) for i in range(nwx - 1)])
    up1, low1 = call(pack_own_kernel, (YROWS, YROWS), vmem(3), [], 16, (st, v0, m), 5_000_000)
    rl1 = lax.ppermute(up1, "ny", up)
    ru1 = lax.ppermute(low1, "ny", down)
    up2, low2, im = call(
        pack_kernel, (YROWS, YROWS, NB * R), vmem(3), [], 16, (rf, rb, m), 5_000_000
    )
    rl2 = lax.ppermute(up2, "ny", up)
    ru2 = lax.ppermute(low2, "ny", down)
    kc, hc, u1, v1 = call(
        functools.partial(slab_kernel, nwx),
        (2 * NB * R, 2 * NB * R, 3 * R, 3 * R), vmem(6), [tall(5 * sh3), tall(3 * R)],
        24, (st, rf, rb, v0, m, im), 50_000_000,
    )
    own, beside = call(
        unpack_kernel, (UNITS_OWN * 8, UNITS_NEXT * 8), vmem(6), [], 16,
        (rl1, ru1, up1, low1, up2, low2), 5_000_000,
    )
    ke, he, s, vel = call(
        functools.partial(edge_kernel, nwx),
        (2 * NB * EDGE, 2 * NB * EDGE, 3 * BLOCK, 3 * BLOCK), vmem(6),
        [tall(5 * qh3), tall(3 * EDGE), tall(5 * EDGE)],
        16, (rl2, ru2, own, beside, u1, v1),
    )
    near = [(i, i ^ 1) for i in range(nwx)]
    far = [(i, i + 1) for i in range(1, nwx - 1, 2)] + [(i + 1, i) for i in range(1, nwx - 1, 2)]
    for n in range(1, STEPS):
        last = n == STEPS - 1
        rb = lax.ppermute(s, "wx", far)
        ra = lax.ppermute(s, "wx", near)
        acc, acc_e = call(
            mid_kernel, (3 * R, 3 * EDGE), vmem(6), [tall(3 * sh3), tall(3 * qh3)],
            16, (s, ra, kc, hc, ke, he), 50_000_000,
        )
        size = 3 * R if last else 3 * BLOCK
        s, vel = call(
            functools.partial(far_kernel, last),
            (size, size), vmem(10),
            [tall(3 * sh3), tall(3 * qh3), tall(3 * R), tall(3 * EDGE)],
            16, (s, ra, rb, vel, acc, acc_e, kc, hc, ke, he),
        )
    back = lambda x: x.reshape(3, Z, X, Y).transpose(0, 2, 1, 3)
    return back(s), back(vel)


def solution(mesh):
    wide = P(None, "wx", None, "ny")
    return jax.shard_map(
        functools.partial(on_device, mesh.shape["wx"], mesh.shape["ny"]),
        mesh=mesh,
        in_specs=(wide, wide, P("wx", None, "ny"), wide, P(), P()),
        out_specs=(wide, wide),
        check_vma=False,
    )
```

```python
import functools
import math

import jax
import jax.numpy as jnp
from jax import lax
from jax.experimental import pallas as pl
from jax.experimental.pallas import tpu as pltpu
from jax.sharding import PartitionSpec as P


STEPS = 3
MATS = 8
DT = 0.05
X, Z, Y = 4, 6, 128
R = X * Z
W = 9
G = 42
SLOTS = 4
F32 = jnp.float32


def bond_offsets():
    out = []
    for a in range(0, 4):
        for b in range(-3, 4):
            for c in range(-3, 4):
                if a * a + b * b + c * c <= 9:
                    if a > 0 or (a == 0 and (b > 0 or (b == 0 and c > 0))):
                        out.append((a, b, c))
    return out


OFFS = bond_offsets()
NB = len(OFFS)
CROSS = [k for k in range(NB) if OFFS[k][0] > 0]


def rows_of(k):
    return OFFS[k][0] * Z + OFFS[k][1]


PREV_AT = {}
_at = 0
for _k in CROSS:
    PREV_AT[_k] = _at
    _at += rows_of(_k)
PREV_ROWS = -(-_at // 8) * 8
STATE0 = 5 * R
UNITS_OWN = 8 + NB
UNITS_NEXT = 10 + NB
YROWS = -(-UNITS_NEXT // SLOTS) * 8
EDGE = 8
BLOCK = R + EDGE


def lanes(rows):
    return lax.broadcasted_iota(jnp.int32, (rows, Y), 1)


def roll(x, shift):
    shift %= Y
    return x if shift == 0 else pltpu.roll(x, shift, axis=1)


def params(n):
    return pltpu.CompilerParams(vmem_limit_bytes=n << 20)


def vmem(n):
    return [pl.BlockSpec(memory_space=pltpu.VMEM)] * n


def shape(rows):
    return jax.ShapeDtypeStruct((rows, Y), F32)


CHUNKS = ((14, 30), (30, 46), (46, NB), (0, 14))


def first_kernel(nwx, nny, *refs):
    given, (st, xf, v0, m_out), local, sems = refs[:6], refs[6:10], refs[10:16], refs[16]
    tmp = refs[17]
    stiff, crit, u, v, lab, mask = local
    copies = [pltpu.make_async_copy(given[i], local[i], sems.at[i]) for i in (0, 1, 2, 4, 3)]
    parts = [
        pltpu.make_async_copy(
            given[5].at[k0 * R : k1 * R, :], mask.at[k0 * R : k1 * R, :], sems.at[5 + i]
        )
        for i, (k0, k1) in enumerate(CHUNKS)
    ]
    for copy in copies[:4] + parts + copies[4:]:
        copy.start()
    wx, ny = lax.axis_index("wx"), lax.axis_index("ny")
    for copy in copies[:4]:
        copy.wait()
    for q in range(3):
        for x in range(X):
            st[q * R + x * Z : q * R + (x + 1) * Z, :] = u[pl.ds(q * R + x, Z, stride=X), :]
    for x in range(X):
        tmp[x * Z : (x + 1) * Z, :] = lab[pl.ds(x, Z, stride=X), :]
    label = tmp[...]
    mod = jnp.zeros((R, Y), F32)
    lim = jnp.zeros((R, Y), F32)
    for t in range(MATS):
        hit = label == t
        mod = jnp.where(hit, stiff[t], mod)
        lim = jnp.where(hit, crit[t], lim)
    st[3 * R : 4 * R, :] = mod
    st[4 * R : 5 * R, :] = lim
    xf[0:STATE0, :] = st[...]
    row = lax.broadcasted_iota(jnp.int32, (R, Y), 0)
    zi = row % Z
    gx = wx * X + row // Z
    gy = ny * Y + lanes(R)
    for part, (k0, k1) in zip(parts, CHUNKS):
        part.wait()
        for k in range(k0, k1):
            a, b, c = OFFS[k]
            for x in range(X):
                m_out[k * R + x * Z : k * R + (x + 1) * Z, :] = mask[
                    pl.ds(k * R + x, Z, stride=X), :
                ].astype(F32)
            ok = (zi + b >= 0) & (zi + b < Z) & (gx + a < nwx * X)
            if c:
                ok = ok & (gy + c >= 0) & (gy + c < nny * Y)
            m_out[k * R : (k + 1) * R, :] = jnp.where(ok, m_out[k * R : (k + 1) * R, :], 0.0)
            if a:
                o, at = rows_of(k), STATE0 + PREV_AT[k]
                xf[at : at + o, :] = m_out[(k + 1) * R - o : (k + 1) * R, :]
    if _at < PREV_ROWS:
        xf[STATE0 + _at : STATE0 + PREV_ROWS, :] = jnp.zeros((PREV_ROWS - _at, Y), F32)
    copies[4].wait()
    for q in range(3):
        for x in range(X):
            v0[q * R + x * Z : q * R + (x + 1) * Z, :] = v[pl.ds(q * R + x, Z, stride=X), :]


def pack_units(unit, units, to_upper, to_lower, first=0, final=YROWS // 8):
    lane = lanes(8)
    for t in range(first, final):
        up = jnp.zeros((8, Y), F32)
        low = jnp.zeros((8, Y), F32)
        for p in range(SLOTS):
            if t * SLOTS + p >= units:
                continue
            value = unit(t * SLOTS + p)
            for g in range(3):
                part = value[8 * g : 8 * g + 8, :]
                at = G * g + W * p
                here = (lane >= at) & (lane < at + W)
                up = jnp.where(here, roll(part, at + W), up)
                low = jnp.where(here, roll(part, at), low)
        to_upper[8 * t : 8 * t + 8, :] = up
        to_lower[8 * t : 8 * t + 8, :] = low


def pack_own_kernel(st, v0, m, to_upper, to_lower):
    def unit(n):
        if n < 5:
            return st[n * R : (n + 1) * R, :]
        if n < 8:
            return v0[(n - 5) * R : (n - 4) * R, :]
        return m[(n - 8) * R : (n - 7) * R, :]

    pack_units(unit, UNITS_OWN, to_upper, to_lower)


SPLIT = (5 + NB) // SLOTS


def pack_kernel(rf, m, to_upper, to_lower, im):
    for k in range(NB):
        o, at = rows_of(k), k * R
        if o == 0:
            im[at : at + R, :] = m[at : at + R, :]
            continue
        if OFFS[k][0]:
            im[at : at + o, :] = rf[STATE0 + PREV_AT[k] : STATE0 + PREV_AT[k] + o, :]
        else:
            im[at : at + o, :] = jnp.zeros((o, Y), F32)
        im[at + o : at + R, :] = m[at : at + R - o, :]

    def unit(n):
        return rf[n * R : (n + 1) * R, :] if n < 5 else im[(n - 5) * R : (n - 4) * R, :]

    pack_units(unit, 5 + NB, to_upper, to_lower, 0, SPLIT)


def pack_rest_kernel(upper, lower, rb, im, to_upper, to_lower):
    to_upper[0 : 8 * SPLIT, :] = upper[...]
    to_lower[0 : 8 * SPLIT, :] = lower[...]

    def unit(n):
        if n < 5 + NB:
            return im[(n - 5) * R : (n - 4) * R, :]
        return rb[(n - 5 - NB) * R : (n - 4 - NB) * R, :]

    pack_units(unit, UNITS_NEXT, to_upper, to_lower, SPLIT)


def group_place(lo, hi):
    place, inside = places()
    return inside & (place >= lo) & (place < hi)


def own_columns(n, mine_up, mine_low, out):
    t, p = n // SLOTS, n % SLOTS
    at = slice(8 * t, 8 * t + 8)
    out = jnp.where(group_place(W, W + OWN), roll(mine_low[at, :], W - W * p), out)
    return jnp.where(group_place(W + OWN, W + 2 * OWN), roll(mine_up[at, :], 2 * OWN - W * p), out)


def outer_columns(n, rl, ru, out):
    t, p = n // SLOTS, n % SLOTS
    at = slice(8 * t, 8 * t + 8)
    out = jnp.where(group_place(0, W), roll(rl[at, :], -W * p), out)
    return jnp.where(
        group_place(W + 2 * OWN, 2 * W + 2 * OWN), roll(ru[at, :], W + 2 * OWN - W * p), out
    )


def unpack_kernel(rl, ru, up1, low1, up2, low2, own, beside):
    zero = jnp.zeros((8, Y), F32)
    for n in range(UNITS_OWN):
        own[8 * n : 8 * n + 8, :] = outer_columns(n, rl, ru, own_columns(n, up1, low1, zero))
    for n in range(UNITS_NEXT):
        beside[8 * n : 8 * n + 8, :] = own_columns(n, up2, low2, zero)


OWN = 6


def places():
    lane = lanes(8)
    return lane % G, lane < 3 * G


def tied(main, edge, with_edge=True):
    lane = lanes(8)
    rows = []
    for g in range(3):
        part = main[8 * g : 8 * g + 8, :]
        low = roll(edge, -(G * g + W))
        high = roll(edge, -(G * g + W + 2 * OWN))
        rows.append(jnp.where(lane < 3, low, jnp.where(lane >= Y - 3, high, part)))
    if with_edge:
        place, inside = places()
        for g in range(3):
            part = main[8 * g : 8 * g + 8, :]
            here = inside & (lane >= G * g) & (lane < G * (g + 1))
            low = here & (place >= W + 3) & (place < W + OWN)
            high = here & (place >= W + OWN) & (place < W + OWN + 3)
            edge = jnp.where(low, roll(part, G * g + W), edge)
            edge = jnp.where(high, roll(part, G * g + W + 2 * OWN), edge)
    return jnp.concatenate(rows, axis=0), edge


def shift_slabs(main, number, sh, first=0, reach=3):
    rows = 3 * R
    for c in range(-reach, reach + 1):
        at = (number * 7 + c + 3) * rows + first
        sh[at : at + main.shape[0], :] = roll(main, -c)


def shift_edges(edges, number, qh, low=0, high=(3 * R - 16) // 8, reach=3):
    q = 3 * R - 16
    lane = lanes(8)
    tiles = []
    for n in range(low, high):
        part = [roll(edges[(n + g) // 3], G * (g - (n + g) % 3)) for g in range(3)]
        tiles.append(jnp.where(lane < G, part[0], jnp.where(lane < 2 * G, part[1], part[2])))
    for c in range(-reach, reach + 1):
        at = (number * 7 + c + 3) * q + 8 * low
        for n, tile in enumerate(tiles):
            qh[at + 8 * n : at + 8 * n + 8, :] = roll(tile, -c)


def slab_at(number, o, c):
    return (number * 7 + c + 3) * 3 * R + R + o


def edge_at(number, o, c):
    return (number * 7 + c + 3) * (3 * R - 16) + R + o


DIRECTED = [(n // 2, 1 - 2 * (n % 2)) for n in range(2 * NB)]
ALL = list(range(2 * NB))


def in_parts(live, numbers, size, fn):
    for start in range(0, len(numbers), size):
        pl.when(live)(functools.partial(fn, numbers[start : start + size]))


def add_forces(numbers, here, shifted, at_of, rows, kc, hc, acc, lo=0, hi=None):
    hi = rows if hi is None else hi
    total = [acc[q * rows + lo : q * rows + hi, :] for q in range(3)]
    mine = [here(q)[lo:hi, :] if (lo, hi) == (0, rows) else here(q, lo, hi) for q in range(3)]
    for n in numbers:
        k, sign = DIRECTED[n]
        a, b, c = OFFS[k]
        length = math.sqrt(a * a + b * b + c * c)
        d = (sign * a, sign * b, sign * c)
        e = []
        for q in range(3):
            at = at_of(q, sign * rows_of(k), d[2])
            there = shifted[at + lo : at + hi, :]
            e.append(there + float(d[q]) - mine[q] if d[q] else there - mine[q])
        sq = e[0] * e[0] + e[1] * e[1] + e[2] * e[2]
        t = sq * lax.rsqrt(jnp.maximum(sq, 1e-36)) - length
        at = n * rows
        mag = kc[at + lo : at + hi, :] * t / (hc[at + lo : at + hi, :] + t * t)
        total = [total[q] + mag * e[q] for q in range(3)]
    for q in range(3):
        acc[q * rows + lo : q * rows + hi, :] = total[q]


def rows_from(ref, stride, start=0):
    def here(q, lo=0, hi=None):
        hi = R if hi is None else hi
        return ref[q * stride + start + lo : q * stride + start + hi, :]

    return here


def edges_from(ref, stride, start=0):
    return lambda q: ref[q * stride + start : q * stride + start + EDGE, :]


def coefficients(mask, m_i, m_j, l_i, l_j, length):
    half = 0.5 * (l_i + l_j)
    sq = half * half
    return mask * (2.0 * m_i * m_j / (m_i + m_j)) * sq * (1.0 / length), sq * (length * length)


def length_of(k):
    a, b, c = OFFS[k]
    return math.sqrt(a * a + b * b + c * c)


def filled(x):
    return jnp.where(x > 0.0, x, 1.0)


PART = 16
PART_EDGE = 32


def slab_kernel(nwx, st, rf, rb, v0, m, im, kc, hc, u1, v1, sh, acc):
    live = lax.axis_index("wx") < nwx
    for q in range(5):
        at = q * R
        main = jnp.concatenate([rf[at : at + R, :], st[at : at + R, :], rb[at : at + R, :]], axis=0)
        shift_slabs(filled(main) if q >= 3 else main, q, sh)
    acc[...] = jnp.zeros_like(acc)

    def part(numbers):
        mod, lim = st[3 * R : 4 * R, :], st[4 * R : 5 * R, :]
        for n in numbers:
            k, sign = DIRECTED[n]
            o, c = sign * rows_of(k), sign * OFFS[k][2]
            mask = m[k * R : (k + 1) * R, :] if sign > 0 else roll(im[k * R : (k + 1) * R, :], -c)
            mj, lj = (sh[slab_at(q, o, c) : slab_at(q, o, c) + R, :] for q in (3, 4))
            kk, hh = coefficients(mask, mod, mj, lim, lj, length_of(k))
            kc[n * R : (n + 1) * R, :] = kk
            hc[n * R : (n + 1) * R, :] = hh
        add_forces(numbers, rows_from(st, R), sh, slab_at, R, kc, hc, acc)

    in_parts(live, ALL, PART, part)
    vel = v0[...] + DT * acc[...]
    v1[...] = vel
    u1[...] = st[0 : 3 * R, :] + DT * vel


def edge_kernel(nwx, rl, ru, own, beside, u1, v1, kc, hc, s_out, v_out, qh, acc, ue):
    live = lax.axis_index("wx") < nwx

    def own_tile(n):
        return own[8 * n : 8 * n + 8, :]

    def tile(n):
        return outer_columns(n, rl, ru, beside[8 * n : 8 * n + 8, :])

    for q in range(5):
        tiles = [tile(q), own_tile(q), tile(5 + NB + q)]
        if q >= 3:
            tiles = [filled(x) for x in tiles]
        ue[8 * q : 8 * q + 8, :] = tiles[1]
        shift_edges(tiles, q, qh)
    acc[...] = jnp.zeros_like(acc)

    def part(numbers):
        mod, lim = ue[24:32, :], ue[32:40, :]
        for n in numbers:
            k, sign = DIRECTED[n]
            o, c = sign * rows_of(k), sign * OFFS[k][2]
            mask = own_tile(8 + k) if sign > 0 else roll(tile(5 + k), -c)
            mj, lj = (qh[edge_at(q, o, c) : edge_at(q, o, c) + EDGE, :] for q in (3, 4))
            kk, hh = coefficients(mask, mod, mj, lim, lj, length_of(k))
            kc[n * EDGE : (n + 1) * EDGE, :] = kk
            hc[n * EDGE : (n + 1) * EDGE, :] = hh
        add_forces(numbers, edges_from(ue, EDGE), qh, edge_at, EDGE, kc, hc, acc)

    in_parts(live, ALL, 64, part)
    for q in range(3):
        vel = own_tile(5 + q) + DT * acc[q * EDGE : (q + 1) * EDGE, :]
        dis = ue[q * EDGE : (q + 1) * EDGE, :] + DT * vel
        finish(q, u1[q * R : (q + 1) * R, :], dis, v1[q * R : (q + 1) * R, :], vel, s_out, v_out)


def finish(q, dis, dis_e, vel, vel_e, s_out, v_out):
    dis, dis_e = tied(dis, dis_e)
    at = q * BLOCK
    s_out[at : at + R, :] = dis
    s_out[at + R : at + BLOCK, :] = dis_e
    v_out[at : at + R, :] = vel
    v_out[at + R : at + BLOCK, :] = vel_e


def toward(sign):
    return {a: [n for n in ALL if DIRECTED[n][1] == sign and OFFS[n // 2][0] == a] for a in (1, 2, 3)}


def mid_kernel(s, near, kc, hc, ke, he, acc, acc_e, sh, qh):
    even = lax.rem(lax.axis_index("wx"), 2) == 0
    acc[...] = jnp.zeros_like(acc)
    acc_e[...] = jnp.zeros_like(acc_e)
    zero = jnp.zeros((EDGE, Y), F32)

    def build(far_sign):
        for q in range(3):
            at = q * BLOCK
            mid, other = s[at : at + BLOCK, :], near[at : at + BLOCK, :]
            if far_sign < 0:
                shift_slabs(jnp.concatenate([zero, mid[:R], other[:R]], axis=0), q, sh, R - 8)
                shift_edges([zero, mid[R:], other[R:]], q, qh, 2, 7)
            else:
                shift_slabs(jnp.concatenate([other[:R], mid[:R], zero], axis=0), q, sh)
                shift_edges([other[R:], mid[R:], zero], q, qh, 0, 5)

    for far_sign, side in ((-1, even), (1, jnp.logical_not(even))):
        pl.when(side)(functools.partial(build, far_sign))
        leaving = toward(far_sign)
        whole = [n for n in ALL if not any(n in x for x in leaving.values())]

        def slab_part(numbers):
            add_forces(numbers, rows_from(s, BLOCK), sh, slab_at, R, kc, hc, acc)

        def edge_part(numbers):
            add_forces(numbers, edges_from(s, BLOCK, R), qh, edge_at, EDGE, ke, he, acc_e)

        in_parts(side, whole, PART, slab_part)
        in_parts(side, whole, PART_EDGE, edge_part)
        for a in (1, 2, 3):
            lo, hi = (Z * a, R) if far_sign < 0 else (0, R - Z * a)

            def inner_part(numbers, lo=lo, hi=hi):
                add_forces(numbers, rows_from(s, BLOCK), sh, slab_at, R, kc, hc, acc, lo, hi)

            in_parts(side, leaving[a], PART, inner_part)


def far_kernel(last, s, near, far, v, part, part_e, kc, hc, ke, he, s_out, v_out, sh, qh, acc, acc_e):
    even = lax.rem(lax.axis_index("wx"), 2) == 0
    acc[...] = part[...]
    acc_e[...] = part_e[...]

    def build(far_sign):
        for q in range(3):
            at = q * BLOCK
            mid, close, other = (x[at : at + BLOCK, :] for x in (s, near, far))
            if far_sign < 0:
                shift_slabs(jnp.concatenate([other[:R], mid[:8]], axis=0), q, sh, 0, 2)
                shift_edges([other[R:], mid[R:], close[R:]], q, qh, 0, 4, 2)
            else:
                shift_slabs(jnp.concatenate([mid[R - 8 : R], other[:R]], axis=0), q, sh, 2 * R - 8, 2)
                shift_edges([close[R:], mid[R:], other[R:]], q, qh, 3, 7, 2)

    def slab_part(lo, hi, numbers):
        add_forces(numbers, rows_from(s, BLOCK), sh, slab_at, R, kc, hc, acc, lo, hi)

    def edge_part(numbers):
        add_forces(numbers, edges_from(s, BLOCK, R), qh, edge_at, EDGE, ke, he, acc_e)

    for far_sign, side in ((-1, even), (1, jnp.logical_not(even))):
        pl.when(side)(functools.partial(build, far_sign))
        leaving = toward(far_sign)
        for a in (1, 2, 3):
            lo, hi = (0, Z * a) if far_sign < 0 else (R - Z * a, R)
            in_parts(side, leaving[a], PART_EDGE, functools.partial(slab_part, lo, hi))
        in_parts(side, leaving[1] + leaving[2] + leaving[3], PART_EDGE, edge_part)
    for q in range(3):
        at = q * BLOCK
        vel = v[at : at + R, :] + DT * acc[q * R : (q + 1) * R, :]
        dis = s[at : at + R, :] + DT * vel
        vel_e = v[at + R : at + BLOCK, :] + DT * acc_e[q * EDGE : (q + 1) * EDGE, :]
        dis_e = s[at + R : at + BLOCK, :] + DT * vel_e
        if not last:
            finish(q, dis, dis_e, vel, vel_e, s_out, v_out)
            continue
        acc[q * R : (q + 1) * R, :] = tied(dis, dis_e, False)[0]
        for x in range(X):
            s_out[pl.ds(q * R + x, Z, stride=X), :] = acc[q * R + x * Z : q * R + (x + 1) * Z, :]
        sh[q * R : (q + 1) * R, :] = tied(vel, vel_e, False)[0]
        for x in range(X):
            v_out[pl.ds(q * R + x, Z, stride=X), :] = sh[q * R + x * Z : q * R + (x + 1) * Z, :]


def call(kernel, outs, specs, scratch, mib, args, flops=0):
    return pl.pallas_call(
        kernel,
        out_shape=tuple(shape(n) for n in outs),
        in_specs=specs,
        out_specs=tuple(vmem(len(outs))),
        scratch_shapes=scratch,
        compiler_params=params(mib),
        cost_estimate=pl.CostEstimate(flops=flops, bytes_accessed=0, transcendentals=0),
    )(*args)


def tall(rows, dtype=F32):
    return pltpu.VMEM((rows, Y), dtype)


def on_device(nwx, nny, displacement, velocity, labels, bond_mask, stiffness, critical):
    flat = lambda x: x.transpose(0, 2, 1, 3).reshape(-1, Y)
    u, v, mask = flat(displacement), flat(velocity), flat(bond_mask)
    lab = labels.transpose(1, 0, 2).reshape(R, Y)
    sh3, qh3 = 7 * 3 * R, 7 * (3 * R - 16)
    i32 = jnp.int32
    st, xf, v0, m = call(
        functools.partial(first_kernel, nwx, nny),
        (STATE0, STATE0 + PREV_ROWS, 3 * R, NB * R),
        [pl.BlockSpec(memory_space=pltpu.HBM)] * 6,
        [pltpu.SMEM((MATS,), F32), pltpu.SMEM((MATS,), F32), tall(3 * R), tall(3 * R),
         tall(R, i32), tall(NB * R, i32), pltpu.SemaphoreType.DMA((5 + len(CHUNKS),)), tall(R, i32)],
        16, tuple(pltpu.with_memory_space_constraint(x, pltpu.HBM) for x in (stiffness, critical, u, v, lab, mask)),
    )
    up = [(i, i + 1) for i in range(nny - 1)]
    down = [(i + 1, i) for i in range(nny - 1)]
    rf = lax.ppermute(xf, "wx", [(i, i + 1) for i in range(nwx - 1)])
    rb = lax.ppermute(st, "wx", [(i + 1, i) for i in range(nwx - 1)])
    up1, low1 = call(pack_own_kernel, (YROWS, YROWS), vmem(3), [], 16, (st, v0, m), 5_000_000)
    rl1 = lax.ppermute(up1, "ny", up)
    ru1 = lax.ppermute(low1, "ny", down)
    up2, low2, im = call(
        pack_kernel, (8 * SPLIT, 8 * SPLIT, NB * R), vmem(2), [], 16, (rf, m),
        5_000_000,
    )
    up2, low2 = call(pack_rest_kernel, (YROWS, YROWS), vmem(4), [], 16, (up2, low2, rb, im))
    rl2 = lax.ppermute(up2, "ny", up)
    ru2 = lax.ppermute(low2, "ny", down)
    kc, hc, u1, v1 = call(
        functools.partial(slab_kernel, nwx),
        (2 * NB * R, 2 * NB * R, 3 * R, 3 * R), vmem(6), [tall(5 * sh3), tall(3 * R)],
        24, (st, rf, rb, v0, m, im), 50_000_000,
    )
    own, beside = call(
        unpack_kernel, (UNITS_OWN * 8, UNITS_NEXT * 8), vmem(6), [], 16,
        (rl1, ru1, up1, low1, up2, low2), 5_000_000,
    )
    ke, he, s, vel = call(
        functools.partial(edge_kernel, nwx),
        (2 * NB * EDGE, 2 * NB * EDGE, 3 * BLOCK, 3 * BLOCK), vmem(6),
        [tall(5 * qh3), tall(3 * EDGE), tall(5 * EDGE)],
        16, (rl2, ru2, own, beside, u1, v1),
    )
    near = [(i, i ^ 1) for i in range(nwx)]
    far = [(i, i + 1) for i in range(1, nwx - 1, 2)] + [(i + 1, i) for i in range(1, nwx - 1, 2)]
    for n in range(1, STEPS):
        last = n == STEPS - 1
        rb = lax.ppermute(s, "wx", far)
        ra = lax.ppermute(s, "wx", near)
        acc, acc_e = call(
            mid_kernel, (3 * R, 3 * EDGE), vmem(6), [tall(3 * sh3), tall(3 * qh3)],
            16, (s, ra, kc, hc, ke, he), 50_000_000,
        )
        size = 3 * R if last else 3 * BLOCK
        s, vel = call(
            functools.partial(far_kernel, last),
            (size, size), vmem(10),
            [tall(3 * sh3), tall(3 * qh3), tall(3 * R), tall(3 * EDGE)],
            16, (s, ra, rb, vel, acc, acc_e, kc, hc, ke, he),
        )
    back = lambda x: x.reshape(3, Z, X, Y).transpose(0, 2, 1, 3)
    return back(s), back(vel)


def solution(mesh):
    wide = P(None, "wx", None, "ny")
    return jax.shard_map(
        functools.partial(on_device, mesh.shape["wx"], mesh.shape["ny"]),
        mesh=mesh,
        in_specs=(wide, wide, P("wx", None, "ny"), wide, P(), P()),
        out_specs=(wide, wide),
        check_vma=False,
    )
```

```python
import functools
import math

import jax
import jax.numpy as jnp
from jax import lax
from jax.experimental import pallas as pl
from jax.experimental.pallas import tpu as pltpu
from jax.sharding import PartitionSpec as P


STEPS = 3
MATS = 8
DT = 0.05
X, Z, Y = 4, 6, 128
R = X * Z
W = 9
G = 42
SLOTS = 4
F32 = jnp.float32


def bond_offsets():
    out = []
    for a in range(0, 4):
        for b in range(-3, 4):
            for c in range(-3, 4):
                if a * a + b * b + c * c <= 9:
                    if a > 0 or (a == 0 and (b > 0 or (b == 0 and c > 0))):
                        out.append((a, b, c))
    return out


OFFS = bond_offsets()
NB = len(OFFS)
CROSS = [k for k in range(NB) if OFFS[k][0] > 0]


def rows_of(k):
    return OFFS[k][0] * Z + OFFS[k][1]


PREV_AT = {}
_at = 0
for _k in CROSS:
    PREV_AT[_k] = _at
    _at += rows_of(_k)
PREV_ROWS = -(-_at // 8) * 8
STATE0 = 5 * R
UNITS_OWN = 8 + NB
UNITS_NEXT = 10 + NB
YROWS = -(-UNITS_NEXT // SLOTS) * 8
EDGE = 8
BLOCK = R + EDGE


def lanes(rows):
    return lax.broadcasted_iota(jnp.int32, (rows, Y), 1)


def roll(x, shift):
    shift %= Y
    return x if shift == 0 else pltpu.roll(x, shift, axis=1)


def params(n):
    return pltpu.CompilerParams(vmem_limit_bytes=n << 20)


def vmem(n):
    return [pl.BlockSpec(memory_space=pltpu.VMEM)] * n


def shape(rows):
    return jax.ShapeDtypeStruct((rows, Y), F32)


CHUNKS = ((14, 30), (30, 46), (46, NB), (0, 14))


def first_kernel(nwx, nny, *refs):
    given, (st, xf, v0, m_out), local, sems = refs[:6], refs[6:10], refs[10:16], refs[16]
    tmp = refs[17]
    stiff, crit, u, v, lab, mask = local
    copies = [pltpu.make_async_copy(given[i], local[i], sems.at[i]) for i in (0, 1, 2, 4, 3)]
    parts = [
        pltpu.make_async_copy(
            given[5].at[k0 * R : k1 * R, :], mask.at[k0 * R : k1 * R, :], sems.at[5 + i]
        )
        for i, (k0, k1) in enumerate(CHUNKS)
    ]
    for copy in copies[:4] + parts + copies[4:]:
        copy.start()
    wx, ny = lax.axis_index("wx"), lax.axis_index("ny")
    for copy in copies[:4]:
        copy.wait()
    for q in range(3):
        for x in range(X):
            st[q * R + x * Z : q * R + (x + 1) * Z, :] = u[pl.ds(q * R + x, Z, stride=X), :]
    for x in range(X):
        tmp[x * Z : (x + 1) * Z, :] = lab[pl.ds(x, Z, stride=X), :]
    label = tmp[...]
    mod = jnp.zeros((R, Y), F32)
    lim = jnp.zeros((R, Y), F32)
    for t in range(MATS):
        hit = label == t
        mod = jnp.where(hit, stiff[t], mod)
        lim = jnp.where(hit, crit[t], lim)
    st[3 * R : 4 * R, :] = mod
    st[4 * R : 5 * R, :] = lim
    xf[0:STATE0, :] = st[...]
    row = lax.broadcasted_iota(jnp.int32, (R, Y), 0)
    zi = row % Z
    gx = wx * X + row // Z
    gy = ny * Y + lanes(R)
    for part, (k0, k1) in zip(parts, CHUNKS):
        part.wait()
        for k in range(k0, k1):
            a, b, c = OFFS[k]
            for x in range(X):
                m_out[k * R + x * Z : k * R + (x + 1) * Z, :] = mask[
                    pl.ds(k * R + x, Z, stride=X), :
                ].astype(F32)
            ok = (zi + b >= 0) & (zi + b < Z) & (gx + a < nwx * X)
            if c:
                ok = ok & (gy + c >= 0) & (gy + c < nny * Y)
            m_out[k * R : (k + 1) * R, :] = jnp.where(ok, m_out[k * R : (k + 1) * R, :], 0.0)
            if a:
                o, at = rows_of(k), STATE0 + PREV_AT[k]
                xf[at : at + o, :] = m_out[(k + 1) * R - o : (k + 1) * R, :]
    if _at < PREV_ROWS:
        xf[STATE0 + _at : STATE0 + PREV_ROWS, :] = jnp.zeros((PREV_ROWS - _at, Y), F32)
    copies[4].wait()
    for q in range(3):
        for x in range(X):
            v0[q * R + x * Z : q * R + (x + 1) * Z, :] = v[pl.ds(q * R + x, Z, stride=X), :]


def pack_units(unit, units, to_upper, to_lower, first=0, final=YROWS // 8):
    lane = lanes(8)
    for t in range(first, final):
        up = jnp.zeros((8, Y), F32)
        low = jnp.zeros((8, Y), F32)
        for p in range(SLOTS):
            if t * SLOTS + p >= units:
                continue
            value = unit(t * SLOTS + p)
            for g in range(3):
                part = value[8 * g : 8 * g + 8, :]
                at = G * g + W * p
                here = (lane >= at) & (lane < at + W)
                up = jnp.where(here, roll(part, at + W), up)
                low = jnp.where(here, roll(part, at), low)
        to_upper[8 * t : 8 * t + 8, :] = up
        to_lower[8 * t : 8 * t + 8, :] = low


def pack_own_kernel(st, v0, m, to_upper, to_lower):
    def unit(n):
        if n < 5:
            return st[n * R : (n + 1) * R, :]
        if n < 8:
            return v0[(n - 5) * R : (n - 4) * R, :]
        return m[(n - 8) * R : (n - 7) * R, :]

    pack_units(unit, UNITS_OWN, to_upper, to_lower)


SPLIT = (5 + NB) // SLOTS


def pack_kernel(rf, m, to_upper, to_lower, im):
    for k in range(NB):
        o, at = rows_of(k), k * R
        if o == 0:
            im[at : at + R, :] = m[at : at + R, :]
            continue
        if OFFS[k][0]:
            im[at : at + o, :] = rf[STATE0 + PREV_AT[k] : STATE0 + PREV_AT[k] + o, :]
        else:
            im[at : at + o, :] = jnp.zeros((o, Y), F32)
        im[at + o : at + R, :] = m[at : at + R - o, :]

    def unit(n):
        return rf[n * R : (n + 1) * R, :] if n < 5 else im[(n - 5) * R : (n - 4) * R, :]

    pack_units(unit, 5 + NB, to_upper, to_lower, 0, SPLIT)


def pack_rest_kernel(upper, lower, rb, im, to_upper, to_lower):
    to_upper[0 : 8 * SPLIT, :] = upper[...]
    to_lower[0 : 8 * SPLIT, :] = lower[...]

    def unit(n):
        if n < 5 + NB:
            return im[(n - 5) * R : (n - 4) * R, :]
        return rb[(n - 5 - NB) * R : (n - 4 - NB) * R, :]

    pack_units(unit, UNITS_NEXT, to_upper, to_lower, SPLIT)


def group_place(lo, hi):
    place, inside = places()
    return inside & (place >= lo) & (place < hi)


def own_columns(n, mine_up, mine_low, out):
    t, p = n // SLOTS, n % SLOTS
    at = slice(8 * t, 8 * t + 8)
    out = jnp.where(group_place(W, W + OWN), roll(mine_low[at, :], W - W * p), out)
    return jnp.where(group_place(W + OWN, W + 2 * OWN), roll(mine_up[at, :], 2 * OWN - W * p), out)


def outer_columns(n, rl, ru, out):
    t, p = n // SLOTS, n % SLOTS
    at = slice(8 * t, 8 * t + 8)
    out = jnp.where(group_place(0, W), roll(rl[at, :], -W * p), out)
    return jnp.where(
        group_place(W + 2 * OWN, 2 * W + 2 * OWN), roll(ru[at, :], W + 2 * OWN - W * p), out
    )


def unpack_kernel(rl, ru, up1, low1, up2, low2, own, beside):
    zero = jnp.zeros((8, Y), F32)
    for n in range(UNITS_OWN):
        own[8 * n : 8 * n + 8, :] = outer_columns(n, rl, ru, own_columns(n, up1, low1, zero))
    for n in range(UNITS_NEXT):
        beside[8 * n : 8 * n + 8, :] = own_columns(n, up2, low2, zero)


OWN = 6


def places():
    lane = lanes(8)
    return lane % G, lane < 3 * G


def tied(main, edge, with_edge=True):
    lane = lanes(8)
    rows = []
    for g in range(3):
        part = main[8 * g : 8 * g + 8, :]
        low = roll(edge, -(G * g + W))
        high = roll(edge, -(G * g + W + 2 * OWN))
        rows.append(jnp.where(lane < 3, low, jnp.where(lane >= Y - 3, high, part)))
    if with_edge:
        place, inside = places()
        for g in range(3):
            part = main[8 * g : 8 * g + 8, :]
            here = inside & (lane >= G * g) & (lane < G * (g + 1))
            low = here & (place >= W + 3) & (place < W + OWN)
            high = here & (place >= W + OWN) & (place < W + OWN + 3)
            edge = jnp.where(low, roll(part, G * g + W), edge)
            edge = jnp.where(high, roll(part, G * g + W + 2 * OWN), edge)
    return jnp.concatenate(rows, axis=0), edge


def shift_slabs(main, number, sh, first=0, reach=3):
    rows = 3 * R
    for c in range(-reach, reach + 1):
        at = (number * 7 + c + 3) * rows + first
        sh[at : at + main.shape[0], :] = roll(main, -c)


def shift_edges(edges, number, qh, low=0, high=(3 * R - 16) // 8, reach=3):
    q = 3 * R - 16
    lane = lanes(8)
    tiles = []
    for n in range(low, high):
        part = [roll(edges[(n + g) // 3], G * (g - (n + g) % 3)) for g in range(3)]
        tiles.append(jnp.where(lane < G, part[0], jnp.where(lane < 2 * G, part[1], part[2])))
    for c in range(-reach, reach + 1):
        at = (number * 7 + c + 3) * q + 8 * low
        for n, tile in enumerate(tiles):
            qh[at + 8 * n : at + 8 * n + 8, :] = roll(tile, -c)


def slab_at(number, o, c):
    return (number * 7 + c + 3) * 3 * R + R + o


def edge_at(number, o, c):
    return (number * 7 + c + 3) * (3 * R - 16) + R + o


DIRECTED = [(n // 2, 1 - 2 * (n % 2)) for n in range(2 * NB)]
ALL = list(range(2 * NB))


def in_parts(live, numbers, size, fn):
    for start in range(0, len(numbers), size):
        pl.when(live)(functools.partial(fn, numbers[start : start + size]))


def add_forces(numbers, here, shifted, at_of, rows, kc, hc, acc, lo=0, hi=None):
    hi = rows if hi is None else hi
    total = [acc[q * rows + lo : q * rows + hi, :] for q in range(3)]
    mine = [here(q)[lo:hi, :] if (lo, hi) == (0, rows) else here(q, lo, hi) for q in range(3)]
    moved = {}
    for n in numbers:
        k, sign = DIRECTED[n]
        a, b, c = OFFS[k]
        length = math.sqrt(a * a + b * b + c * c)
        d = (sign * a, sign * b, sign * c)
        e = []
        for q in range(3):
            at = at_of(q, sign * rows_of(k), d[2])
            there = shifted[at + lo : at + hi, :]
            if (q, d[q]) not in moved:
                moved[q, d[q]] = mine[q] - float(d[q]) if d[q] else mine[q]
            e.append(there - moved[q, d[q]])
        sq = e[0] * e[0] + e[1] * e[1] + e[2] * e[2]
        t = sq * lax.rsqrt(jnp.maximum(sq, 1e-36)) - length
        at = n * rows
        mag = kc[at + lo : at + hi, :] * t / (hc[at + lo : at + hi, :] + t * t)
        total = [total[q] + mag * e[q] for q in range(3)]
    for q in range(3):
        acc[q * rows + lo : q * rows + hi, :] = total[q]


def rows_from(ref, stride, start=0):
    def here(q, lo=0, hi=None):
        hi = R if hi is None else hi
        return ref[q * stride + start + lo : q * stride + start + hi, :]

    return here


def edges_from(ref, stride, start=0):
    return lambda q: ref[q * stride + start : q * stride + start + EDGE, :]


def coefficients(mask, m_i, m_j, l_i, l_j, length):
    half = 0.5 * (l_i + l_j)
    sq = half * half
    return mask * (2.0 * m_i * m_j / (m_i + m_j)) * sq * (1.0 / length), sq * (length * length)


def length_of(k):
    a, b, c = OFFS[k]
    return math.sqrt(a * a + b * b + c * c)


def filled(x):
    return jnp.where(x > 0.0, x, 1.0)


PART = 16
PART_EDGE = 32


def slab_kernel(nwx, st, rf, rb, v0, m, im, kc, hc, u1, v1, sh, acc):
    live = lax.axis_index("wx") < nwx
    for q in range(5):
        at = q * R
        main = jnp.concatenate([rf[at : at + R, :], st[at : at + R, :], rb[at : at + R, :]], axis=0)
        shift_slabs(filled(main) if q >= 3 else main, q, sh)
    acc[...] = jnp.zeros_like(acc)

    def part(numbers):
        mod, lim = st[3 * R : 4 * R, :], st[4 * R : 5 * R, :]
        for n in numbers:
            k, sign = DIRECTED[n]
            o, c = sign * rows_of(k), sign * OFFS[k][2]
            mask = m[k * R : (k + 1) * R, :] if sign > 0 else roll(im[k * R : (k + 1) * R, :], -c)
            mj, lj = (sh[slab_at(q, o, c) : slab_at(q, o, c) + R, :] for q in (3, 4))
            kk, hh = coefficients(mask, mod, mj, lim, lj, length_of(k))
            kc[n * R : (n + 1) * R, :] = kk
            hc[n * R : (n + 1) * R, :] = hh
        add_forces(numbers, rows_from(st, R), sh, slab_at, R, kc, hc, acc)

    in_parts(live, ALL, PART, part)
    vel = v0[...] + DT * acc[...]
    v1[...] = vel
    u1[...] = st[0 : 3 * R, :] + DT * vel


def edge_kernel(nwx, rl, ru, own, beside, u1, v1, kc, hc, s_out, v_out, qh, acc, ue):
    live = lax.axis_index("wx") < nwx

    def own_tile(n):
        return own[8 * n : 8 * n + 8, :]

    def tile(n):
        return outer_columns(n, rl, ru, beside[8 * n : 8 * n + 8, :])

    for q in range(5):
        tiles = [tile(q), own_tile(q), tile(5 + NB + q)]
        if q >= 3:
            tiles = [filled(x) for x in tiles]
        ue[8 * q : 8 * q + 8, :] = tiles[1]
        shift_edges(tiles, q, qh)
    acc[...] = jnp.zeros_like(acc)

    def part(numbers):
        mod, lim = ue[24:32, :], ue[32:40, :]
        for n in numbers:
            k, sign = DIRECTED[n]
            o, c = sign * rows_of(k), sign * OFFS[k][2]
            mask = own_tile(8 + k) if sign > 0 else roll(tile(5 + k), -c)
            mj, lj = (qh[edge_at(q, o, c) : edge_at(q, o, c) + EDGE, :] for q in (3, 4))
            kk, hh = coefficients(mask, mod, mj, lim, lj, length_of(k))
            kc[n * EDGE : (n + 1) * EDGE, :] = kk
            hc[n * EDGE : (n + 1) * EDGE, :] = hh
        add_forces(numbers, edges_from(ue, EDGE), qh, edge_at, EDGE, kc, hc, acc)

    in_parts(live, ALL, 64, part)
    for q in range(3):
        vel = own_tile(5 + q) + DT * acc[q * EDGE : (q + 1) * EDGE, :]
        dis = ue[q * EDGE : (q + 1) * EDGE, :] + DT * vel
        finish(q, u1[q * R : (q + 1) * R, :], dis, v1[q * R : (q + 1) * R, :], vel, s_out, v_out)


def finish(q, dis, dis_e, vel, vel_e, s_out, v_out):
    dis, dis_e = tied(dis, dis_e)
    at = q * BLOCK
    s_out[at : at + R, :] = dis
    s_out[at + R : at + BLOCK, :] = dis_e
    v_out[at : at + R, :] = vel
    v_out[at + R : at + BLOCK, :] = vel_e


def toward(sign):
    return {a: [n for n in ALL if DIRECTED[n][1] == sign and OFFS[n // 2][0] == a] for a in (1, 2, 3)}


def mid_kernel(s, near, kc, hc, ke, he, acc, acc_e, sh, qh):
    even = lax.rem(lax.axis_index("wx"), 2) == 0
    acc[...] = jnp.zeros_like(acc)
    acc_e[...] = jnp.zeros_like(acc_e)
    zero = jnp.zeros((EDGE, Y), F32)

    def build(far_sign):
        for q in range(3):
            at = q * BLOCK
            mid, other = s[at : at + BLOCK, :], near[at : at + BLOCK, :]
            if far_sign < 0:
                shift_slabs(jnp.concatenate([zero, mid[:R], other[:R]], axis=0), q, sh, R - 8)
                shift_edges([zero, mid[R:], other[R:]], q, qh, 2, 7)
            else:
                shift_slabs(jnp.concatenate([other[:R], mid[:R], zero], axis=0), q, sh)
                shift_edges([other[R:], mid[R:], zero], q, qh, 0, 5)

    for far_sign, side in ((-1, even), (1, jnp.logical_not(even))):
        pl.when(side)(functools.partial(build, far_sign))
        leaving = toward(far_sign)
        whole = [n for n in ALL if not any(n in x for x in leaving.values())]

        def slab_part(numbers):
            add_forces(numbers, rows_from(s, BLOCK), sh, slab_at, R, kc, hc, acc)

        def edge_part(numbers):
            add_forces(numbers, edges_from(s, BLOCK, R), qh, edge_at, EDGE, ke, he, acc_e)

        in_parts(side, whole, PART, slab_part)
        in_parts(side, whole, PART_EDGE, edge_part)
        for a in (1, 2, 3):
            lo, hi = (Z * a, R) if far_sign < 0 else (0, R - Z * a)

            def inner_part(numbers, lo=lo, hi=hi):
                add_forces(numbers, rows_from(s, BLOCK), sh, slab_at, R, kc, hc, acc, lo, hi)

            in_parts(side, leaving[a], PART, inner_part)


def far_kernel(last, s, near, far, v, part, part_e, kc, hc, ke, he, s_out, v_out, sh, qh, acc, acc_e):
    even = lax.rem(lax.axis_index("wx"), 2) == 0
    acc[...] = part[...]
    acc_e[...] = part_e[...]

    def build(far_sign):
        for q in range(3):
            at = q * BLOCK
            mid, close, other = (x[at : at + BLOCK, :] for x in (s, near, far))
            if far_sign < 0:
                shift_slabs(jnp.concatenate([other[:R], mid[:8]], axis=0), q, sh, 0, 2)
                shift_edges([other[R:], mid[R:], close[R:]], q, qh, 0, 4, 2)
            else:
                shift_slabs(jnp.concatenate([mid[R - 8 : R], other[:R]], axis=0), q, sh, 2 * R - 8, 2)
                shift_edges([close[R:], mid[R:], other[R:]], q, qh, 3, 7, 2)

    def slab_part(lo, hi, numbers):
        add_forces(numbers, rows_from(s, BLOCK), sh, slab_at, R, kc, hc, acc, lo, hi)

    def edge_part(numbers):
        add_forces(numbers, edges_from(s, BLOCK, R), qh, edge_at, EDGE, ke, he, acc_e)

    for far_sign, side in ((-1, even), (1, jnp.logical_not(even))):
        pl.when(side)(functools.partial(build, far_sign))
        leaving = toward(far_sign)
        for a in (1, 2, 3):
            lo, hi = (0, Z * a) if far_sign < 0 else (R - Z * a, R)
            in_parts(side, leaving[a], PART_EDGE, functools.partial(slab_part, lo, hi))
        in_parts(side, leaving[1] + leaving[2] + leaving[3], PART_EDGE, edge_part)
    for q in range(3):
        at = q * BLOCK
        vel = v[at : at + R, :] + DT * acc[q * R : (q + 1) * R, :]
        dis = s[at : at + R, :] + DT * vel
        vel_e = v[at + R : at + BLOCK, :] + DT * acc_e[q * EDGE : (q + 1) * EDGE, :]
        dis_e = s[at + R : at + BLOCK, :] + DT * vel_e
        if not last:
            finish(q, dis, dis_e, vel, vel_e, s_out, v_out)
            continue
        acc[q * R : (q + 1) * R, :] = tied(dis, dis_e, False)[0]
        for x in range(X):
            s_out[pl.ds(q * R + x, Z, stride=X), :] = acc[q * R + x * Z : q * R + (x + 1) * Z, :]
        sh[q * R : (q + 1) * R, :] = tied(vel, vel_e, False)[0]
        for x in range(X):
            v_out[pl.ds(q * R + x, Z, stride=X), :] = sh[q * R + x * Z : q * R + (x + 1) * Z, :]


def call(kernel, outs, specs, scratch, mib, args, flops=0):
    return pl.pallas_call(
        kernel,
        out_shape=tuple(shape(n) for n in outs),
        in_specs=specs,
        out_specs=tuple(vmem(len(outs))),
        scratch_shapes=scratch,
        compiler_params=params(mib),
        cost_estimate=pl.CostEstimate(flops=flops, bytes_accessed=0, transcendentals=0),
    )(*args)


def tall(rows, dtype=F32):
    return pltpu.VMEM((rows, Y), dtype)


def on_device(nwx, nny, displacement, velocity, labels, bond_mask, stiffness, critical):
    flat = lambda x: x.transpose(0, 2, 1, 3).reshape(-1, Y)
    u, v, mask = flat(displacement), flat(velocity), flat(bond_mask)
    lab = labels.transpose(1, 0, 2).reshape(R, Y)
    sh3, qh3 = 7 * 3 * R, 7 * (3 * R - 16)
    i32 = jnp.int32
    st, xf, v0, m = call(
        functools.partial(first_kernel, nwx, nny),
        (STATE0, STATE0 + PREV_ROWS, 3 * R, NB * R),
        [pl.BlockSpec(memory_space=pltpu.HBM)] * 6,
        [pltpu.SMEM((MATS,), F32), pltpu.SMEM((MATS,), F32), tall(3 * R), tall(3 * R),
         tall(R, i32), tall(NB * R, i32), pltpu.SemaphoreType.DMA((5 + len(CHUNKS),)), tall(R, i32)],
        16, tuple(pltpu.with_memory_space_constraint(x, pltpu.HBM) for x in (stiffness, critical, u, v, lab, mask)),
    )
    up = [(i, i + 1) for i in range(nny - 1)]
    down = [(i + 1, i) for i in range(nny - 1)]
    rf = lax.ppermute(xf, "wx", [(i, i + 1) for i in range(nwx - 1)])
    rb = lax.ppermute(st, "wx", [(i + 1, i) for i in range(nwx - 1)])
    up1, low1 = call(pack_own_kernel, (YROWS, YROWS), vmem(3), [], 16, (st, v0, m), 5_000_000)
    rl1 = lax.ppermute(up1, "ny", up)
    ru1 = lax.ppermute(low1, "ny", down)
    up2, low2, im = call(
        pack_kernel, (8 * SPLIT, 8 * SPLIT, NB * R), vmem(2), [], 16, (rf, m),
        5_000_000,
    )
    up2, low2 = call(pack_rest_kernel, (YROWS, YROWS), vmem(4), [], 16, (up2, low2, rb, im))
    rl2 = lax.ppermute(up2, "ny", up)
    ru2 = lax.ppermute(low2, "ny", down)
    kc, hc, u1, v1 = call(
        functools.partial(slab_kernel, nwx),
        (2 * NB * R, 2 * NB * R, 3 * R, 3 * R), vmem(6), [tall(5 * sh3), tall(3 * R)],
        24, (st, rf, rb, v0, m, im), 50_000_000,
    )
    own, beside = call(
        unpack_kernel, (UNITS_OWN * 8, UNITS_NEXT * 8), vmem(6), [], 16,
        (rl1, ru1, up1, low1, up2, low2), 5_000_000,
    )
    ke, he, s, vel = call(
        functools.partial(edge_kernel, nwx),
        (2 * NB * EDGE, 2 * NB * EDGE, 3 * BLOCK, 3 * BLOCK), vmem(6),
        [tall(5 * qh3), tall(3 * EDGE), tall(5 * EDGE)],
        16, (rl2, ru2, own, beside, u1, v1),
    )
    near = [(i, i ^ 1) for i in range(nwx)]
    far = [(i, i + 1) for i in range(1, nwx - 1, 2)] + [(i + 1, i) for i in range(1, nwx - 1, 2)]
    for n in range(1, STEPS):
        last = n == STEPS - 1
        rb = lax.ppermute(s, "wx", far)
        ra = lax.ppermute(s, "wx", near)
        acc, acc_e = call(
            mid_kernel, (3 * R, 3 * EDGE), vmem(6), [tall(3 * sh3), tall(3 * qh3)],
            16, (s, ra, kc, hc, ke, he), 50_000_000,
        )
        size = 3 * R if last else 3 * BLOCK
        s, vel = call(
            functools.partial(far_kernel, last),
            (size, size), vmem(10),
            [tall(3 * sh3), tall(3 * qh3), tall(3 * R), tall(3 * EDGE)],
            16, (s, ra, rb, vel, acc, acc_e, kc, hc, ke, he),
        )
    back = lambda x: x.reshape(3, Z, X, Y).transpose(0, 2, 1, 3)
    return back(s), back(vel)


def solution(mesh):
    wide = P(None, "wx", None, "ny")
    return jax.shard_map(
        functools.partial(on_device, mesh.shape["wx"], mesh.shape["ny"]),
        mesh=mesh,
        in_specs=(wide, wide, P("wx", None, "ny"), wide, P(), P()),
        out_specs=(wide, wide),
        check_vma=False,
    )
```
